8 devices in a mesh: dp: 2 (over z, y), ctx: 4 (over x, core).
Axes of the slice: x: 2, y: 2, z: 1, core: 2. Of those that a mesh axis runs over, the one named last changes fastest.
Arguments:
- queries: bfloat16 [64, 512, 12, 128], P('dp', 'ctx'), parts along dimension 0
- keys: bfloat16 [64, 512, 1, 128], P('dp', 'ctx'), parts along dimension 0
- values: bfloat16 [64, 512, 1, 128], P('dp', 'ctx'), parts along dimension 0
- grad_out: bfloat16 [64, 512, 12, 128], P('dp', 'ctx'), parts along dimension 0
Outputs:
- output 1: bfloat16 [64, 512, 12, 128], P('dp', 'ctx'), parts along dimension 0
- output 2: bfloat16 [64, 512, 12, 128], P('dp', 'ctx'), parts along dimension 0
- output 3: bfloat16 [64, 512, 1, 128], P('dp', 'ctx'), parts along dimension 0
- output 4: bfloat16 [64, 512, 1, 128], P('dp', 'ctx'), parts along dimension 0
There are 2 independent parts. The reference program is written for one: setup_inputs(seed, part) draws one part's arguments, and reference() takes and returns one part's arrays. A program takes and returns all parts, laid end to end along the dimension named above; each array names one.
All inputs are finite; a program needn't handle non-finite values.
Results may differ from the reference program's by a relative error of at most 0.0071199.
Values are sent between devices in bfloat16 or wider.
A program may use at most 1 GiB of HBM per device.

```python
import jax
import jax.numpy as jnp
from jax import lax

BATCH = 32
SEQ = 512
HQ = 12
HEAD_DIM = 128
BLOCK = 128
NEG_BIG = -1e30


def setup_inputs(seed: int = 0, part: int = 0) -> dict:
    part_key = jax.random.fold_in(jax.random.key(seed), part)
    key_q, key_k, key_v, key_do = jax.random.split(part_key, 4)
    q_shape = (BATCH, SEQ, HQ, HEAD_DIM)
    kv_shape = (BATCH, SEQ, 1, HEAD_DIM)
    queries = 1.5 * jax.random.normal(key_q, q_shape, jnp.float32)
    keys = jax.random.normal(key_k, kv_shape, jnp.float32)
    values = jax.random.normal(key_v, kv_shape, jnp.float32)
    grad_out = jax.random.normal(key_do, q_shape, jnp.float32)
    return {"queries": queries.astype(jnp.bfloat16), "keys": keys.astype(jnp.bfloat16), "values": values.astype(jnp.bfloat16), "grad_out": grad_out.astype(jnp.bfloat16)}


def reference(queries, keys, values, grad_out):
    n_kv = keys.shape[2]
    n_grp = HQ // n_kv
    n_blocks = SEQ // BLOCK
    scale = HEAD_DIM ** -0.5
    q_lead = jnp.moveaxis(queries.reshape(BATCH, n_blocks, BLOCK, n_kv, n_grp, HEAD_DIM), 1, 0)
    do_lead = jnp.moveaxis(grad_out.reshape(BATCH, n_blocks, BLOCK, n_kv, n_grp, HEAD_DIM), 1, 0)
    k_blocks = keys.reshape(BATCH, n_blocks, BLOCK, n_kv, HEAD_DIM)
    v_blocks = values.reshape(BATCH, n_blocks, BLOCK, n_kv, HEAD_DIM)
    blk_ids = jnp.arange(n_blocks)
    stat_shape = (BATCH, n_kv, n_grp, BLOCK)

    def block_scores(q_blk, k_blk, blk_idx, key_idx):
        scores = jnp.einsum("bihgd,bjhd->bhgij", q_blk.astype(jnp.float32), k_blk.astype(jnp.float32)) * scale
        q_pos = blk_idx * BLOCK + jnp.arange(BLOCK)
        k_pos = key_idx * BLOCK + jnp.arange(BLOCK)
        return jnp.where(q_pos[:, None] >= k_pos[None, :], scores, NEG_BIG)

    def forward_block(inputs):
        q_blk, blk_idx = inputs

        def loop_body(key_idx, carry):
            m_run, l_run, acc_run = carry
            k_blk = lax.dynamic_index_in_dim(k_blocks, key_idx, 1, keepdims=False)
            v_blk = lax.dynamic_index_in_dim(v_blocks, key_idx, 1, keepdims=False)
            scores = block_scores(q_blk, k_blk, blk_idx, key_idx)
            m_new = jnp.maximum(m_run, scores.max(axis=-1))
            rescale = jnp.exp(m_run - m_new)
            weights = jnp.exp(scores - m_new[..., None])
            l_new = l_run * rescale + weights.sum(axis=-1)
            w_half = weights.astype(jnp.bfloat16).astype(jnp.float32)
            acc_new = acc_run * rescale[..., None] + jnp.einsum("bhgij,bjhd->bhgid", w_half, v_blk.astype(jnp.float32))
            return m_new, l_new, acc_new

        init_carry = (jnp.full(stat_shape, NEG_BIG, jnp.float32), jnp.zeros(stat_shape, jnp.float32), jnp.zeros(stat_shape + (HEAD_DIM,), jnp.float32))
        m_fin, l_fin, acc_fin = lax.fori_loop(0, blk_idx + 1, loop_body, init_carry)
        out_blk = jnp.transpose((acc_fin / l_fin[..., None]).astype(jnp.bfloat16), (0, 3, 1, 2, 4))
        return out_blk, m_fin + jnp.log(l_fin)

    out_lead, lse_lead = lax.map(forward_block, (q_lead, blk_ids))

    def backward_block(carry, inputs):
        dk_acc, dv_acc = carry
        q_blk, do_blk, out_blk, lse_blk, blk_idx = inputs
        q_f = q_blk.astype(jnp.float32)
        do_f = do_blk.astype(jnp.float32)
        delta_row = jnp.einsum("bihgd,bihgd->bhgi", do_f, out_blk.astype(jnp.float32))

        def loop_body(key_idx, inner):
            dq_run, dk_run, dv_run = inner
            k_blk = lax.dynamic_index_in_dim(k_blocks, key_idx, 1, keepdims=False)
            v_blk = lax.dynamic_index_in_dim(v_blocks, key_idx, 1, keepdims=False)
            scores = block_scores(q_blk, k_blk, blk_idx, key_idx)
            weights = jnp.exp(scores - lse_blk[..., None])
            w_half = weights.astype(jnp.bfloat16).astype(jnp.float32)
            dp_blk = jnp.einsum("bihgd,bjhd->bhgij", do_f, v_blk.astype(jnp.float32))
            ds_half = (weights * (dp_blk - delta_row[..., None])).astype(jnp.bfloat16).astype(jnp.float32)
            dq_run = dq_run + jnp.einsum("bhgij,bjhd->bihgd", ds_half, k_blk.astype(jnp.float32))
            dk_old = lax.dynamic_index_in_dim(dk_run, key_idx, 1, keepdims=False)
            dv_old = lax.dynamic_index_in_dim(dv_run, key_idx, 1, keepdims=False)
            dk_new = dk_old + jnp.einsum("bhgij,bihgd->bjhd", ds_half, q_f)
            dv_new = dv_old + jnp.einsum("bhgij,bihgd->bjhd", w_half, do_f)
            dk_run = lax.dynamic_update_index_in_dim(dk_run, dk_new, key_idx, 1)
            dv_run = lax.dynamic_update_index_in_dim(dv_run, dv_new, key_idx, 1)
            return dq_run, dk_run, dv_run

        dq_blk, dk_acc, dv_acc = lax.fori_loop(0, blk_idx + 1, loop_body, (jnp.zeros(q_f.shape, jnp.float32), dk_acc, dv_acc))
        return (dk_acc, dv_acc), dq_blk

    acc_zero = jnp.zeros((BATCH, n_blocks, BLOCK, n_kv, HEAD_DIM), jnp.float32)
    grads, dq_lead = lax.scan(backward_block, (acc_zero, acc_zero), (q_lead, do_lead, out_lead, lse_lead, blk_ids))
    attn_out = jnp.moveaxis(out_lead, 0, 1).reshape(BATCH, SEQ, HQ, HEAD_DIM)
    grad_q = (jnp.moveaxis(dq_lead, 0, 1) * scale).astype(jnp.bfloat16).reshape(BATCH, SEQ, HQ, HEAD_DIM)
    grad_k = (grads[0] * scale).astype(jnp.bfloat16).reshape(BATCH, SEQ, n_kv, HEAD_DIM)
    grad_v = grads[1].astype(jnp.bfloat16).reshape(BATCH, SEQ, n_kv, HEAD_DIM)
    return attn_out, grad_q, grad_k, grad_v
```

```python
import functools

import jax
import jax.numpy as jnp
from jax import lax
from jax.experimental import pallas as pl
from jax.experimental.pallas import tpu as pltpu
from jax.sharding import PartitionSpec as P

F32, BF16 = jnp.float32, jnp.bfloat16
LOG2E = 1.4426950408889634
NEG_BIG = -1e30
MESH = pl.DeviceIdType.MESH
RELAY_AHEAD = 2


def dot(a, b):
    return lax.dot_general(a, b, (((1,), (0,)), ((), ())), preferred_element_type=F32)


def remote(src, dst, send_sem, recv_sem, to):
    return pltpu.make_async_remote_copy(src_ref=src, dst_ref=dst, send_sem=send_sem, recv_sem=recv_sem, device_id={"ctx": to}, device_id_type=MESH)


def device_program(me, n_batch, scale, refs):
    (q_hbm, do_hbm, k_hbm, v_hbm, o_hbm, dq_hbm, dk_hbm, dv_hbm,
     kv, acc, part_a, part_b, grads, q_buf, do_buf, o_buf, dq_buf,
     s_0, s_1, p_0, p_1, dp_0, dp_1, ph_0, ph_1, ds_0, ds_1, max_s, inv_s, kt, vt,
     own_sem, kv_sem, kv_send, pa_sem, pb_sem, pa_send, pb_send, red_send,
     q_sem, do_sem, o_sem, dq_sem, dk_sem) = refs
    blocks = me + 1
    width = blocks * 128
    s_buf, p_buf, dp_buf, ph_buf, ds_buf = (s_0, s_1), (p_0, p_1), (dp_0, dp_1), (ph_0, ph_1), (ds_0, ds_1)
    own = pl.ds(me * 128, 128)

    def rows(j):
        return pl.ds(j * 128, 128)

    def own_copy(a, src):
        return pltpu.make_async_copy(src, kv.at[a, :, own], own_sem.at[a])

    def kv_push(a, src, j, b, to, slot):
        return remote(src, kv.at[a, b, rows(j)], kv_send.at[slot, a], kv_sem.at[a, j, b], to)

    def kv_wait(j, b):
        for a in range(2):
            kv_push(a, kv.at[a, b, rows(j)], j, b, me, 0).wait_recv()

    def q_copy(b, slot):
        return pltpu.make_async_copy(q_hbm.at[b], q_buf.at[slot], q_sem.at[slot])

    def do_copy(b, slot):
        return pltpu.make_async_copy(do_hbm.at[b], do_buf.at[slot], do_sem.at[slot])

    def o_copy(b, slot):
        return pltpu.make_async_copy(o_buf.at[slot], o_hbm.at[b], o_sem.at[slot])

    def dq_copy(b, slot):
        return pltpu.make_async_copy(dq_buf.at[slot], dq_hbm.at[b], dq_sem.at[slot])

    def part_push(j, b, dst, send_sem, recv_sem, to):
        return remote(acc.at[b, :, rows(j)], dst.at[b], send_sem, recv_sem.at[b], to)

    first_hop = {0: [], 1: [(0, part_a, pa_send, pa_sem, 0)], 2: [(1, part_a, pa_send, pa_sem, 3)], 3: [(0, part_a, pa_send, pa_sem, 2), (2, part_b, pb_send, pb_sem, 2)]}[me]
    second_hop = {0: None, 1: None, 2: (0, 0), 3: (1, 1)}[me]
    relay = {0: None, 1: None, 2: (0, 3), 3: (1, 2)}[me]

    def relay_block(b):
        j, to = relay
        kv_wait(j, b)
        for a in range(2):
            kv_push(a, kv.at[a, b, rows(j)], j, b, to, 1).start()

    q_copy(0, 0).start()
    do_copy(0, 0).start()
    own_copy(0, k_hbm).start()
    own_copy(1, v_hbm).start()
    direct = {0: (2, 1), 1: (3,), 2: (3,), 3: ()}[me]
    if direct:

        def push_own(b, carry):
            for slot, to in enumerate(direct):
                for a, src in enumerate((k_hbm, v_hbm)):
                    kv_push(a, src.at[b], me, b, to, 2 * slot).start()
            return carry

        lax.fori_loop(0, n_batch, push_own, 0)
    own_copy(0, k_hbm).wait()
    own_copy(1, v_hbm).wait()
    if relay is not None:
        for b in range(RELAY_AHEAD):
            relay_block(b)

    causal_r = lax.broadcasted_iota(jnp.int32, (128, 256), 0)
    causal_c = lax.broadcasted_iota(jnp.int32, (128, 256), 1) & 127

    def pair(ref, slot, x):
        return ref[slot, 2 * x:2 * x + 2].reshape(256, 128)

    def sub_step(sl, one, two, three):
        so = 1 - sl
        if three is not None:
            b3, acc3, slot3, x3 = three
            q3, do3, o3 = pair(q_buf, slot3[0], x3), pair(do_buf, slot3[0], x3), pair(o_buf, slot3[0], x3)
            delta = jnp.sum((do3.astype(F32) * o3.astype(F32)).T, axis=0, keepdims=True)
            inv3 = inv_s[sl, 0:1]
        if two is not None:
            b2, slot2, x2 = two
            max2 = max_s[so, 0:1]
            dot2 = pair(do_buf, slot2[0], x2).T
        if one is not None:
            b1, slot1, x1 = one
            qt1 = pair(q_buf, slot1[0], x1).T
        max8 = sum8 = None
        for j in range(blocks):
            r = slice(j * 128, j * 128 + 128)
            if two is not None:
                p = jnp.exp2((s_buf[so][r] - max2) * (scale * LOG2E))
                p_buf[so][r] = p
                ph_buf[so][r] = p.astype(BF16)
                part = jnp.sum(p.reshape(16, 8, 256), axis=0)
                sum8 = part if sum8 is None else sum8 + part
            if one is not None:
                st = dot(kv[0, b1, r], qt1)
                if j == blocks - 1:
                    st = jnp.where(causal_r <= causal_c, st, NEG_BIG)
                s_buf[sl][r] = st
                part = jnp.max(st.reshape(16, 8, 256), axis=0)
                max8 = part if max8 is None else jnp.maximum(max8, part)
        if two is not None:
            inv = 1.0 / jnp.sum(sum8, axis=0, keepdims=True)
            inv_s[so, 0:1] = inv
            ot = (dot(vt[slot2[1], :, :width], ph_buf[so][:width]) * inv).astype(BF16)
            o_buf[slot2[0], 2 * x2:2 * x2 + 2] = ot.T.reshape(2, 128, 128)
        if one is not None:
            max_s[sl, 0:1] = jnp.max(max8, axis=0, keepdims=True)
        for j in range(blocks):
            r = slice(j * 128, j * 128 + 128)
            if three is not None:
                pb = p_buf[sl][r] * inv3
                ds = (pb * (dp_buf[sl][r] - delta)).astype(BF16)
                ds_buf[sl][r] = ds
                dv = dot(pb.astype(BF16), do3)
                dk = dot(ds, q3)
                if x3 == 0:
                    acc[acc3, 0, r] = dk
                    acc[acc3, 1, r] = dv
                else:
                    acc[acc3, 0, r] += dk
                    acc[acc3, 1, r] += dv
            if two is not None:
                dp_buf[so][r] = dot(kv[1, b2, r], dot2)
        if three is not None:
            dq = (dot(kt[slot3[1], :, :width], ds_buf[sl][:width]) * scale).astype(BF16)
            dq_buf[slot3[0], 2 * x3:2 * x3 + 2] = dq.T.reshape(2, 128, 128)

    def reduce_part(b):
        j, _ = second_hop
        part_push(j, b, part_a, pa_send, pa_sem, me).wait_recv()
        acc[b, :, rows(j)] += part_a[b]

    def send_reduced(b):
        j, to = second_hop
        part_push(j, b, part_b, red_send, pb_sem, to).start()

    def finish(b, slot):
        o_copy(b, slot).start()
        dq_copy(b, slot).start()
        for hop in first_hop:
            part_push(hop[0], b, hop[1], hop[2], hop[3], hop[4]).start()

    def step(b, carry):
        cur, prev = lax.rem(b, 3), lax.rem(b + 2, 3)
        tcur, tprev = lax.rem(b, 2), lax.rem(b + 1, 2)
        b_prev = jnp.maximum(b - 1, 0)
        acc_prev = jnp.where(b == 0, n_batch, b - 1)

        @pl.when(b + 1 < n_batch)
        def _():
            nxt = lax.rem(b + 1, 3)
            q_copy(b + 1, nxt).start()
            do_copy(b + 1, nxt).start()

        @pl.when(b >= 3)
        def _():
            o_copy(b - 3, cur).wait()
            dq_copy(b - 3, cur).wait()

        if relay is not None:

            @pl.when(b + RELAY_AHEAD < n_batch)
            def _():
                relay_block(b + RELAY_AHEAD)

        for j in range(me):
            if relay is None or j != relay[0]:
                kv_wait(j, b)
        q_copy(b, cur).wait()
        do_copy(b, cur).wait()
        kt[tcur, :, :width] = kv[0, b, :width].T
        vt[tcur, :, :width] = kv[1, b, :width].T
        for x in range(6):
            two = (b_prev, (prev, tprev), 5) if x == 0 else (b, (cur, tcur), x - 1)
            three = (b_prev, acc_prev, (prev, tprev), x + 4) if x < 2 else (b, b, (cur, tcur), x - 2)
            sub_step(x % 2, (b, (cur, tcur), x), two, three)

        if second_hop is not None:

            @pl.when(b >= 2)
            def _():
                reduce_part(b - 2)

        @pl.when(b >= 1)
        def _():
            finish(b - 1, prev)

        if second_hop is not None:

            @pl.when(b >= 2)
            def _():
                send_reduced(b - 2)

        return carry

    lax.fori_loop(0, n_batch, step, 0)

    last = n_batch - 1
    ls, lt = last % 3, last % 2
    sub_step(0, None, (last, (ls, lt), 5), (last, last, (ls, lt), 4))
    sub_step(1, None, None, (last, last, (ls, lt), 5))
    if second_hop is not None:
        reduce_part(last - 1)
    finish(last, ls)
    if second_hop is not None:
        send_reduced(last - 1)
        reduce_part(last)
        send_reduced(last)

    def finalize(b, carry):
        total = acc[b, :, own]
        if me == 0:
            part_push(0, b, part_a, pa_send, pa_sem, me).wait_recv()
            total = total + part_a[b]
        if me < 3:
            part_push(0, b, part_b, pb_send, pb_sem, me).wait_recv()
            total = total + part_b[b]
        grads[b, 0] = (total[0] * scale).astype(BF16)
        grads[b, 1] = total[1].astype(BF16)
        pltpu.make_async_copy(grads.at[b, 0], dk_hbm.at[b], dk_sem.at[0]).start()
        pltpu.make_async_copy(grads.at[b, 1], dv_hbm.at[b], dk_sem.at[1]).start()
        return carry

    lax.fori_loop(0, n_batch, finalize, 0)

    for b in range(n_batch - 3, n_batch):
        o_copy(b, b % 3).wait()
        dq_copy(b, b % 3).wait()
    pltpu.make_async_copy(grads.at[:, 0], dk_hbm, dk_sem.at[0]).wait()
    pltpu.make_async_copy(grads.at[:, 1], dv_hbm, dk_sem.at[1]).wait()
    for slot in range(len(direct)):
        for a, src in enumerate((k_hbm, v_hbm)):
            remote(src, kv.at[a, :, own], kv_send.at[2 * slot, a], kv_sem.at[a, 0, 0], me).wait_send()
    if relay is not None:
        for a in range(2):
            remote(kv.at[a, :, rows(relay[0])], kv.at[a, :, own], kv_send.at[1, a], kv_sem.at[a, 0, 0], me).wait_send()
    every = pl.ds(0, n_batch)
    for j, dst, send_sem, _, _ in first_hop:
        remote(acc.at[every, :, rows(j)], dst, send_sem, pa_sem.at[0], me).wait_send()
    if second_hop is not None:
        remote(acc.at[every, :, rows(second_hop[0])], part_b, red_send, pa_sem.at[0], me).wait_send()


def kernel(n_ctx, n_batch, scale, *refs):
    me = lax.axis_index("ctx")
    barrier = pltpu.get_barrier_semaphore()
    for step in range(1, n_ctx):
        pl.semaphore_signal(barrier, inc=1, device_id={"ctx": lax.rem(me + step, n_ctx)}, device_id_type=MESH)
    pl.semaphore_wait(barrier, n_ctx - 1)
    for i in range(n_ctx):
        pl.when(me == i)(functools.partial(device_program, i, n_batch, scale, refs))


def solution(mesh):
    part_spec = P("dp", "ctx")
    n_ctx = mesh.shape["ctx"]

    def local_step(queries, keys, values, grad_out):
        n_batch, c_len, n_q, d_head = queries.shape
        heads = (0, 2, 1, 3)
        q, do = jnp.transpose(queries, heads), jnp.transpose(grad_out, heads)
        k, v = keys.reshape(n_batch, c_len, d_head), values.reshape(n_batch, c_len, d_head)
        width = n_ctx * c_len
        vmem, dma = pltpu.VMEM, pltpu.SemaphoreType.DMA
        scratch = [
            vmem((2, n_batch, width, d_head), BF16),
            vmem((n_batch + 1, 2, width, d_head), F32),
            vmem((n_batch, 2, c_len, d_head), F32),
            vmem((n_batch, 2, c_len, d_head), F32),
            vmem((n_batch, 2, c_len, d_head), BF16),
        ]
        scratch += [vmem((3, n_q, c_len, d_head), BF16)] * 4
        scratch += [vmem((width, 256), F32)] * 6 + [vmem((width, 256), BF16)] * 4
        scratch += [vmem((2, 8, 256), F32)] * 2 + [vmem((2, d_head, width), BF16)] * 2
        scratch += [dma((2,)), dma((2, n_ctx, n_batch)), dma((3, 2)), dma((n_batch,)), dma((n_batch,)), dma, dma, dma]
        scratch += [dma((3,))] * 4 + [dma((2,))]
        hbm = pl.BlockSpec(memory_space=pl.ANY)
        out_q, out_k = jax.ShapeDtypeStruct(q.shape, BF16), jax.ShapeDtypeStruct(k.shape, BF16)
        out, grad_q, grad_k, grad_v = pl.pallas_call(
            functools.partial(kernel, n_ctx, n_batch, d_head ** -0.5),
            out_shape=[out_q, out_q, out_k, out_k],
            in_specs=[hbm] * 4,
            out_specs=[hbm] * 4,
            scratch_shapes=scratch,
            compiler_params=pltpu.CompilerParams(collective_id=0, has_side_effects=True, vmem_limit_bytes=62 * 2 ** 20),
        )(q, do, k, v)
        return jnp.transpose(out, heads), jnp.transpose(grad_q, heads), grad_k.reshape(keys.shape), grad_v.reshape(values.shape)

    return jax.shard_map(local_step, mesh=mesh, in_specs=(part_spec,) * 4, out_specs=(part_spec,) * 4, check_vma=False)
```

```python
import functools

import jax
import jax.numpy as jnp
from jax import lax
from jax.experimental import pallas as pl
from jax.experimental.pallas import tpu as pltpu
from jax.sharding import PartitionSpec as P

F32, BF16 = jnp.float32, jnp.bfloat16
LOG2E = 1.4426950408889634
NEG_BIG = -1e30
MESH = pl.DeviceIdType.MESH
RELAY_AHEAD = 1
PIECE = 32


def dot(a, b):
    return lax.dot_general(a, b, (((1,), (0,)), ((), ())), preferred_element_type=F32)


def remote(src, dst, send_sem, recv_sem, to):
    return pltpu.make_async_remote_copy(src_ref=src, dst_ref=dst, send_sem=send_sem, recv_sem=recv_sem, device_id={"ctx": to}, device_id_type=MESH)


def device_program(me, n_batch, scale, refs):
    (q_hbm, do_hbm, k_hbm, v_hbm, o_hbm, dq_hbm, dk_hbm, dv_hbm,
     kv, acc, part_a, part_b, grads, q_buf, do_buf, o_buf, dq_buf,
     s_0, s_1, p_0, p_1, p_2, dp_0, dp_1, ph_0, ph_1, ds_0, ds_1, pb_buf, max_s, inv_s, delta_s, kt, vt,
     own_sem, kv_sem, kv_send, pa_sem, pb_sem, pa_send, pb_send, red_send,
     q_sem, do_sem, o_sem, dq_sem, dk_sem) = refs
    blocks = me + 1
    width = blocks * 128
    s_buf, p_buf, dp_buf, ph_buf, ds_buf = (s_0, s_1), (p_0, p_1, p_2), (dp_0, dp_1), (ph_0, ph_1), (ds_0, ds_1)
    own = pl.ds(me * 128, 128)

    def rows(j):
        return pl.ds(j * 128, 128)

    def own_copy(a, src):
        return pltpu.make_async_copy(src, kv.at[a, :, own], own_sem.at[a])

    def kv_push(a, src, j, b, to, slot):
        return remote(src, kv.at[a, b, rows(j)], kv_send.at[slot, a], kv_sem.at[a, j, b], to)

    def kv_wait(j, b):
        for a in range(2):
            kv_push(a, kv.at[a, b, rows(j)], j, b, me, 0).wait_recv()

    def q_copy(b, slot):
        return pltpu.make_async_copy(q_hbm.at[b], q_buf.at[slot], q_sem.at[slot])

    def do_copy(b, slot):
        return pltpu.make_async_copy(do_hbm.at[b], do_buf.at[slot], do_sem.at[slot])

    def o_copy(b, slot):
        return pltpu.make_async_copy(o_buf.at[slot], o_hbm.at[b], o_sem.at[slot])

    def dq_copy(b, slot):
        return pltpu.make_async_copy(dq_buf.at[slot], dq_hbm.at[b], dq_sem.at[slot])

    def part_push(j, b, dst, send_sem, recv_sem, to):
        return remote(acc.at[b, :, rows(j)], dst.at[b], send_sem, recv_sem.at[b], to)

    first_hop = {0: [], 1: [(0, part_a, pa_send, pa_sem, 0)], 2: [(1, part_a, pa_send, pa_sem, 3)], 3: [(0, part_a, pa_send, pa_sem, 2), (2, part_b, pb_send, pb_sem, 2)]}[me]
    second_hop = {0: None, 1: None, 2: (0, 0), 3: (1, 1)}[me]
    relay = {0: None, 1: None, 2: (0, 3), 3: (1, 2)}[me]

    def relay_block(b):
        j, to = relay
        kv_wait(j, b)
        for a in range(2):
            kv_push(a, kv.at[a, b, rows(j)], j, b, to, 1).start()

    q_copy(0, 0).start()
    do_copy(0, 0).start()
    own_copy(0, k_hbm).start()
    own_copy(1, v_hbm).start()
    direct = {0: (2, 1), 1: (3,), 2: (3,), 3: ()}[me]
    if direct:

        def push_own(b, carry):
            for slot, to in enumerate(direct):
                for a, src in enumerate((k_hbm, v_hbm)):
                    kv_push(a, src.at[b], me, b, to, 2 * slot).start()
            return carry

        lax.fori_loop(0, n_batch, push_own, 0)
    own_copy(0, k_hbm).wait()
    own_copy(1, v_hbm).wait()
    if relay is not None:
        for b in range(RELAY_AHEAD):
            relay_block(b)

    causal_r = lax.broadcasted_iota(jnp.int32, (128, 256), 0)
    causal_c = lax.broadcasted_iota(jnp.int32, (128, 256), 1) & 127

    def pair(ref, slot, x):
        return ref[slot, 2 * x:2 * x + 2].reshape(256, 128)

    def sub_step(x, stages):
        par = [(x - k) % 2 for k in range(5)]
        tri = [(x - k) % 3 for k in range(5)]
        s0, s1, s2, s3, s4 = stages
        if s0 is not None:
            qt0 = pair(q_buf, s0[2], s0[4]).T
        if s2 is not None:
            dot2 = pair(do_buf, s2[2], s2[4]).T
        if s1 is not None:
            max1 = max_s[par[1], 0:1]
        if s3 is not None:
            q3, do3 = pair(q_buf, s3[2], s3[4]), pair(do_buf, s3[2], s3[4])
            inv3, delta3 = inv_s[tri[3], 0:1], delta_s[par[3], 0:1]
        max8 = sum8 = None
        for j in range(blocks):
            r = slice(j * 128, j * 128 + 128)
            pieces = [slice(y, y + PIECE) for y in range(j * 128, j * 128 + 128, PIECE)]
            if j == 0 and s2 is not None:
                ot = (dot(vt[s2[3], :, :width], ph_buf[par[2]][:width]) * inv_s[tri[2], 0:1]).astype(BF16)
                o_buf[s2[2], 2 * s2[4]:2 * s2[4] + 2] = ot.T.reshape(2, 128, 128)
                delta_s[par[2], 0:1] = jnp.sum(dot2.astype(F32) * ot.astype(F32), axis=0, keepdims=True)
            if j == min(1, blocks - 1) and s4 is not None:
                dq = (dot(kt[s4[3], :, :width], ds_buf[par[4]][:width]) * scale).astype(BF16)
                dq_buf[s4[2], 2 * s4[4]:2 * s4[4] + 2] = dq.T.reshape(2, 128, 128)
            if s3 is not None:
                for y in pieces:
                    pb = p_buf[tri[3]][y] * inv3
                    ds_buf[par[3]][y] = (pb * (dp_buf[par[3]][y] - delta3)).astype(BF16)
                    pb_buf[y] = pb.astype(BF16)
                dv = dot(pb_buf[r], do3)
                dk = dot(ds_buf[par[3]][r], q3)
                if s3[4] == 0:
                    acc[s3[1], 0, r] = dk
                    acc[s3[1], 1, r] = dv
                else:
                    acc[s3[1], 0, r] += dk
                    acc[s3[1], 1, r] += dv
            if s0 is not None:
                st = dot(kv[0, s0[0], r], qt0)
                if j == blocks - 1:
                    st = jnp.where(causal_r <= causal_c, st, NEG_BIG)
                s_buf[par[0]][r] = st
                part = jnp.max(st.reshape(16, 8, 256), axis=0)
                max8 = part if max8 is None else jnp.maximum(max8, part)
            if s1 is not None:
                for y in pieces:
                    p = jnp.exp2((s_buf[par[1]][y] - max1) * (scale * LOG2E))
                    p_buf[tri[1]][y] = p
                    ph_buf[par[1]][y] = p.astype(BF16)
                    part = jnp.sum(p.reshape(PIECE // 8, 8, 256), axis=0)
                    sum8 = part if sum8 is None else sum8 + part
            if s2 is not None:
                dp_buf[par[2]][r] = dot(kv[1, s2[0], r], dot2)
        if s1 is not None:
            inv_s[tri[1], 0:1] = 1.0 / jnp.sum(sum8, axis=0, keepdims=True)
        if s0 is not None:
            max_s[par[0], 0:1] = jnp.max(max8, axis=0, keepdims=True)

    def reduce_part(b):
        j, _ = second_hop
        part_push(j, b, part_a, pa_send, pa_sem, me).wait_recv()
        acc[b, :, rows(j)] += part_a[b]

    def send_reduced(b):
        j, to = second_hop
        part_push(j, b, part_b, red_send, pb_sem, to).start()

    def send_parts(b):
        for j, dst, send_sem, recv_sem, to in first_hop:
            part_push(j, b, dst, send_sem, recv_sem, to).start()

    lag = 1 if me == 3 else 3

    def step(b, carry):
        cur, prev = lax.rem(b, 3), lax.rem(b + 2, 3)
        tcur, tprev = lax.rem(b, 2), lax.rem(b + 1, 2)
        b_prev = jnp.maximum(b - 1, 0)
        acc_prev = jnp.where(b == 0, n_batch, b - 1)

        @pl.when(b + 1 < n_batch)
        def _():
            nxt = lax.rem(b + 1, 3)
            q_copy(b + 1, nxt).start()
            do_copy(b + 1, nxt).start()

        @pl.when(b >= 3)
        def _():
            o_copy(b - 3, cur).wait()
            dq_copy(b - 3, cur).wait()

        if relay is not None:

            @pl.when(b + RELAY_AHEAD < n_batch)
            def _():
                relay_block(b + RELAY_AHEAD)

        for j in range(me):
            if relay is None or j != relay[0]:
                kv_wait(j, b)
        q_copy(b, cur).wait()
        do_copy(b, cur).wait()
        kt[tcur, :, :width] = kv[0, b, :width].T
        vt[tcur, :, :width] = kv[1, b, :width].T
        for x in range(6):
            here = (b, b, cur, tcur)
            before = (b_prev, acc_prev, prev, tprev)
            sub_step(x, [here + (x - k,) if x >= k else before + (x - k + 6,) for k in range(5)])
        pl.when(b >= 1)(lambda: send_parts(b - 1))
        if second_hop is not None:
            pl.when(b >= lag)(lambda: reduce_part(b - lag))

        @pl.when(b >= 1)
        def _():
            o_copy(b - 1, prev).start()
            dq_copy(b - 1, prev).start()

        if second_hop is not None:
            pl.when(b >= lag)(lambda: send_reduced(b - lag))
        return carry

    lax.fori_loop(0, n_batch, step, 0)

    last = n_batch - 1
    ls = last % 3
    end = (last, last, ls, last % 2)
    for x in range(3):
        sub_step(x, [end + (x - k + 6,) if k > x else None for k in range(5)])
    send_parts(last)
    if me == 3:
        reduce_part(last)
    sub_step(3, [None, None, None, None, end + (5,)])
    if me == 3:
        send_reduced(last)
    o_copy(last, ls).start()
    dq_copy(last, ls).start()
    if me == 2:
        for b in range(n_batch - lag, n_batch):
            reduce_part(b)
            send_reduced(b)

    def finalize(b, carry):
        total = acc[b, :, own]
        if me == 0:
            part_push(0, b, part_a, pa_send, pa_sem, me).wait_recv()
            total = total + part_a[b]
        if me < 3:
            part_push(0, b, part_b, pb_send, pb_sem, me).wait_recv()
            total = total + part_b[b]
        grads[b, 0] = (total[0] * scale).astype(BF16)
        grads[b, 1] = total[1].astype(BF16)
        pltpu.make_async_copy(grads.at[b, 0], dk_hbm.at[b], dk_sem.at[0]).start()
        pltpu.make_async_copy(grads.at[b, 1], dv_hbm.at[b], dk_sem.at[1]).start()
        return carry

    lax.fori_loop(0, n_batch, finalize, 0)

    for b in range(n_batch - 3, n_batch):
        o_copy(b, b % 3).wait()
        dq_copy(b, b % 3).wait()
    pltpu.make_async_copy(grads.at[:, 0], dk_hbm, dk_sem.at[0]).wait()
    pltpu.make_async_copy(grads.at[:, 1], dv_hbm, dk_sem.at[1]).wait()
    for slot in range(len(direct)):
        for a, src in enumerate((k_hbm, v_hbm)):
            remote(src, kv.at[a, :, own], kv_send.at[2 * slot, a], kv_sem.at[a, 0, 0], me).wait_send()
    if relay is not None:
        for a in range(2):
            remote(kv.at[a, :, rows(relay[0])], kv.at[a, :, own], kv_send.at[1, a], kv_sem.at[a, 0, 0], me).wait_send()
    every = pl.ds(0, n_batch)
    for j, dst, send_sem, _, _ in first_hop:
        remote(acc.at[every, :, rows(j)], dst, send_sem, pa_sem.at[0], me).wait_send()
    if second_hop is not None:
        remote(acc.at[every, :, rows(second_hop[0])], part_b, red_send, pa_sem.at[0], me).wait_send()


def kernel(n_ctx, n_batch, scale, *refs):
    me = lax.axis_index("ctx")
    barrier = pltpu.get_barrier_semaphore()
    for step in range(1, n_ctx):
        pl.semaphore_signal(barrier, inc=1, device_id={"ctx": lax.rem(me + step, n_ctx)}, device_id_type=MESH)
    pl.semaphore_wait(barrier, n_ctx - 1)
    for i in range(n_ctx):
        pl.when(me == i)(functools.partial(device_program, i, n_batch, scale, refs))


def solution(mesh):
    part_spec = P("dp", "ctx")
    n_ctx = mesh.shape["ctx"]

    def local_step(queries, keys, values, grad_out):
        n_batch, c_len, n_q, d_head = queries.shape
        heads = (0, 2, 1, 3)
        q, do = jnp.transpose(queries, heads), jnp.transpose(grad_out, heads)
        k, v = keys.reshape(n_batch, c_len, d_head), values.reshape(n_batch, c_len, d_head)
        width = n_ctx * c_len
        vmem, dma = pltpu.VMEM, pltpu.SemaphoreType.DMA
        scratch = [
            vmem((2, n_batch, width, d_head), BF16),
            vmem((n_batch + 1, 2, width, d_head), F32),
            vmem((n_batch, 2, c_len, d_head), F32),
            vmem((n_batch, 2, c_len, d_head), F32),
            vmem((n_batch, 2, c_len, d_head), BF16),
        ]
        scratch += [vmem((3, n_q, c_len, d_head), BF16)] * 4
        scratch += [vmem((width, 256), F32)] * 7 + [vmem((width, 256), BF16)] * 5
        scratch += [vmem((2, 8, 256), F32), vmem((3, 8, 256), F32), vmem((2, 8, 256), F32)] + [vmem((2, d_head, width), BF16)] * 2
        scratch += [dma((2,)), dma((2, n_ctx, n_batch)), dma((3, 2)), dma((n_batch,)), dma((n_batch,)), dma, dma, dma]
        scratch += [dma((3,))] * 4 + [dma((2,))]
        hbm = pl.BlockSpec(memory_space=pl.ANY)
        out_q, out_k = jax.ShapeDtypeStruct(q.shape, BF16), jax.ShapeDtypeStruct(k.shape, BF16)
        out, grad_q, grad_k, grad_v = pl.pallas_call(
            functools.partial(kernel, n_ctx, n_batch, d_head ** -0.5),
            out_shape=[out_q, out_q, out_k, out_k],
            in_specs=[hbm] * 4,
            out_specs=[hbm] * 4,
            scratch_shapes=scratch,
            compiler_params=pltpu.CompilerParams(collective_id=0, has_side_effects=True, vmem_limit_bytes=62 * 2 ** 20),
        )(q, do, k, v)
        return jnp.transpose(out, heads), jnp.transpose(grad_q, heads), grad_k.reshape(keys.shape), grad_v.reshape(values.shape)

    return jax.shard_map(local_step, mesh=mesh, in_specs=(part_spec,) * 4, out_specs=(part_spec,) * 4, check_vma=False)
```

```python
import functools

import jax
import jax.numpy as jnp
from jax import lax
from jax.experimental import pallas as pl
from jax.experimental.pallas import tpu as pltpu
from jax.sharding import PartitionSpec as P

F32, BF16 = jnp.float32, jnp.bfloat16
LOG2E = 1.4426950408889634
NEG_BIG = -1e30
MESH = pl.DeviceIdType.MESH
RELAY_AHEAD = 1
RING = 8
CHUNKS = 4
PIECE = 32


def dot(a, b):
    return lax.dot_general(a, b, (((1,), (0,)), ((), ())), preferred_element_type=F32)


def remote(src, dst, send_sem, recv_sem, to):
    return pltpu.make_async_remote_copy(src_ref=src, dst_ref=dst, send_sem=send_sem, recv_sem=recv_sem, device_id={"ctx": to}, device_id_type=MESH)


def device_program(me, n_batch, scale, refs):
    (q_hbm, do_hbm, k_hbm, v_hbm, o_out, dq_out, dk_out, dv_out,
     kv, own_acc, ring, part_a, part_b, q_buf, do_buf,
     s_0, s_1, p_0, p_1, p_2, dp_0, dp_1, ph_0, ph_1, ds_0, ds_1, pb_buf, max_s, inv_s, delta_s, kt, vt,
     own_sem, kv_sem, kv_send, pa_sem, pb_sem, pa_send, pb_send, red_send,
     q_sem, do_sem) = refs
    blocks = me + 1
    width = blocks * 128
    s_buf, p_buf, dp_buf, ph_buf, ds_buf = (s_0, s_1), (p_0, p_1, p_2), (dp_0, dp_1), (ph_0, ph_1), (ds_0, ds_1)
    own = pl.ds(me * 128, 128)

    def rows(j):
        return pl.ds(j * 128, 128)

    def own_copy(a, src):
        return pltpu.make_async_copy(src, kv.at[a, :, own], own_sem.at[a])

    def kv_push(a, src, j, b, to, slot):
        return remote(src, kv.at[a, b, rows(j)], kv_send.at[slot, a], kv_sem.at[a, j, b], to)

    def kv_wait(j, b):
        for a in range(2):
            kv_push(a, kv.at[a, b, rows(j)], j, b, me, 0).wait_recv()

    def q_copy(b, slot):
        return pltpu.make_async_copy(q_hbm.at[b], q_buf.at[slot], q_sem.at[slot])

    def do_copy(b, slot):
        return pltpu.make_async_copy(do_hbm.at[b], do_buf.at[slot], do_sem.at[slot])

    def part_push(j, b, dst, send_sem, recv_sem, to):
        slot = lax.rem(b, RING) if not isinstance(b, int) else b % RING
        return remote(ring.at[slot, :, rows(j)], dst.at[b], send_sem.at[slot], recv_sem.at[b], to)

    first_hop = {0: [], 1: [(0, part_a, pa_send, pa_sem, 0)], 2: [(1, part_a, pa_send, pa_sem, 3)], 3: [(0, part_a, pa_send, pa_sem, 2), (2, part_b, pb_send, pb_sem, 2)]}[me]
    second_hop = {0: None, 1: None, 2: (0, 0), 3: (1, 1)}[me]
    relay = {0: None, 1: None, 2: (0, 3), 3: (1, 2)}[me]

    def relay_block(b):
        j, to = relay
        kv_wait(j, b)
        for a in range(2):
            kv_push(a, kv.at[a, b, rows(j)], j, b, to, 1).start()

    q_copy(0, 0).start()
    do_copy(0, 0).start()
    own_copy(0, k_hbm).start()
    own_copy(1, v_hbm).start()
    direct = {0: (2, 1), 1: (3,), 2: (3,), 3: ()}[me]
    if direct:

        def push_own(b, carry):
            for slot, to in enumerate(direct):
                for a, src in enumerate((k_hbm, v_hbm)):
                    kv_push(a, src.at[b], me, b, to, 2 * slot).start()
            return carry

        lax.fori_loop(0, n_batch, push_own, 0)
    own_copy(0, k_hbm).wait()
    own_copy(1, v_hbm).wait()
    if relay is not None:
        for b in range(RELAY_AHEAD):
            relay_block(b)

    causal_r = lax.broadcasted_iota(jnp.int32, (128, 256), 0)
    causal_c = lax.broadcasted_iota(jnp.int32, (128, 256), 1) & 127

    def pair(ref, slot, x):
        return ref[slot, 2 * x:2 * x + 2].reshape(256, 128)

    def sub_step(x, stages):
        par = [(x - k) % 2 for k in range(5)]
        tri = [(x - k) % 3 for k in range(5)]
        s0, s1, s2, s3, s4 = stages
        if s0 is not None:
            qt0 = pair(q_buf, s0[3], s0[5]).T
        if s2 is not None:
            dot2 = pair(do_buf, s2[3], s2[5]).T
        if s1 is not None:
            max1 = max_s[par[1], 0:1]
        if s3 is not None:
            q3, do3 = pair(q_buf, s3[3], s3[5]), pair(do_buf, s3[3], s3[5])
            inv3, delta3 = inv_s[tri[3], 0:1], delta_s[par[3], 0:1]
        max8 = sum8 = None
        for j in range(blocks):
            r = slice(j * 128, j * 128 + 128)
            pieces = [slice(y, y + PIECE) for y in range(j * 128, j * 128 + 128, PIECE)]
            if j == 0 and s2 is not None:
                ot = (dot(vt[s2[4], :, :width], ph_buf[par[2]][:width]) * inv_s[tri[2], 0:1]).astype(BF16)
                o_out[s2[0], 2 * s2[5]:2 * s2[5] + 2] = ot.T.reshape(2, 128, 128)
                delta_s[par[2], 0:1] = jnp.sum(dot2.astype(F32) * ot.astype(F32), axis=0, keepdims=True)
            if j == min(1, blocks - 1) and s4 is not None:
                dq = (dot(kt[s4[4], :, :width], ds_buf[par[4]][:width]) * scale).astype(BF16)
                dq_out[s4[0], 2 * s4[5]:2 * s4[5] + 2] = dq.T.reshape(2, 128, 128)
            if s3 is not None:
                for y in pieces:
                    pb = p_buf[tri[3]][y] * inv3
                    ds_buf[par[3]][y] = (pb * (dp_buf[par[3]][y] - delta3)).astype(BF16)
                    pb_buf[y] = pb.astype(BF16)
                dv = dot(pb_buf[r], do3)
                dk = dot(ds_buf[par[3]][r], q3)
                for w, part in enumerate((dk, dv)):
                    dst, at = (own_acc, (s3[1], w)) if j == me else (ring, (s3[2], w, r))
                    dst[at] = part if s3[5] == 0 else dst[at] + part
            if s0 is not None:
                st = dot(kv[0, s0[0], r], qt0)
                if j == blocks - 1:
                    st = jnp.where(causal_r <= causal_c, st, NEG_BIG)
                s_buf[par[0]][r] = st
                part = jnp.max(st.reshape(16, 8, 256), axis=0)
                max8 = part if max8 is None else jnp.maximum(max8, part)
            if s1 is not None:
                for y in pieces:
                    p = jnp.exp2((s_buf[par[1]][y] - max1) * (scale * LOG2E))
                    p_buf[tri[1]][y] = p
                    ph_buf[par[1]][y] = p.astype(BF16)
                    part = jnp.sum(p.reshape(PIECE // 8, 8, 256), axis=0)
                    sum8 = part if sum8 is None else sum8 + part
            if s2 is not None:
                dp_buf[par[2]][r] = dot(kv[1, s2[0], r], dot2)
        if s1 is not None:
            inv_s[tri[1], 0:1] = 1.0 / jnp.sum(sum8, axis=0, keepdims=True)
        if s0 is not None:
            max_s[par[0], 0:1] = jnp.max(max8, axis=0, keepdims=True)

    def reduce_part(b):
        j, _ = second_hop
        part_push(j, b, part_a, pa_send, pa_sem, me).wait_recv()
        slot = lax.rem(b, RING) if not isinstance(b, int) else b % RING
        ring[slot, :, rows(j)] += part_a[b]

    def send_reduced(b):
        j, to = second_hop
        part_push(j, b, part_b, red_send, pb_sem, to).start()

    def send_parts(b):
        for j, dst, send_sem, recv_sem, to in first_hop:
            part_push(j, b, dst, send_sem, recv_sem, to).start()

    def sent(b):
        for j, dst, send_sem, recv_sem, to in first_hop:
            part_push(j, b, dst, send_sem, recv_sem, to).wait_send()
        if second_hop is not None:
            part_push(second_hop[0], b, part_b, red_send, pb_sem, second_hop[1]).wait_send()

    lag = 1 if me == 3 else 3

    def step(b, carry):
        cur, prev = lax.rem(b, 3), lax.rem(b + 2, 3)
        tcur, tprev = lax.rem(b, 2), lax.rem(b + 1, 2)
        b_prev = jnp.maximum(b - 1, 0)
        own_prev = jnp.where(b == 0, n_batch, b - 1)
        ring_cur, ring_prev = lax.rem(b, RING), lax.rem(b + RING - 1, RING)

        @pl.when(b + 1 < n_batch)
        def _():
            nxt = lax.rem(b + 1, 3)
            q_copy(b + 1, nxt).start()
            do_copy(b + 1, nxt).start()

        if me > 0:
            pl.when(b >= RING)(lambda: sent(b - RING))

        if relay is not None:

            @pl.when(b + RELAY_AHEAD < n_batch)
            def _():
                relay_block(b + RELAY_AHEAD)

        for j in range(me):
            if relay is None or j != relay[0]:
                kv_wait(j, b)
        q_copy(b, cur).wait()
        do_copy(b, cur).wait()
        kt[tcur, :, :width] = kv[0, b, :width].T
        vt[tcur, :, :width] = kv[1, b, :width].T
        for x in range(6):
            here = (b, b, ring_cur, cur, tcur)
            before = (b_prev, own_prev, ring_prev, prev, tprev)
            sub_step(x, [here + (x - k,) if x >= k else before + (x - k + 6,) for k in range(5)])
        pl.when(b >= 1)(lambda: send_parts(b - 1))
        if second_hop is not None:
            pl.when(b >= lag)(lambda: reduce_part(b - lag))

        if second_hop is not None:
            pl.when(b >= lag)(lambda: send_reduced(b - lag))
        return carry

    lax.fori_loop(0, n_batch, step, 0)

    last = n_batch - 1
    ls = last % 3
    end = (last, last, last % RING, ls, last % 2)
    for x in range(3):
        sub_step(x, [end + (x - k + 6,) if k > x else None for k in range(5)])
    send_parts(last)
    if me == 3:
        reduce_part(last)
    sub_step(3, [None, None, None, None, end + (5,)])
    if me == 3:
        send_reduced(last)
    if me == 2:
        for b in range(n_batch - lag, n_batch):
            reduce_part(b)
            send_reduced(b)

    def finalize(b, carry):
        total = own_acc[b]
        if me == 0:
            part_push(0, b, part_a, pa_send, pa_sem, me).wait_recv()
            total = total + part_a[b]
        if me < 3:
            part_push(0, b, part_b, pb_send, pb_sem, me).wait_recv()
            total = total + part_b[b]
        dk_out[b] = (total[0] * scale).astype(BF16)
        dv_out[b] = total[1].astype(BF16)
        return carry

    lax.fori_loop(0, n_batch, finalize, 0)

    if me > 0:
        for b in range(n_batch - RING, n_batch):
            sent(b)
    for slot in range(len(direct)):
        for a, src in enumerate((k_hbm, v_hbm)):
            remote(src, kv.at[a, :, own], kv_send.at[2 * slot, a], kv_sem.at[a, 0, 0], me).wait_send()
    if relay is not None:
        for a in range(2):
            remote(kv.at[a, :, rows(relay[0])], kv.at[a, :, own], kv_send.at[1, a], kv_sem.at[a, 0, 0], me).wait_send()


def kernel(n_ctx, n_batch, scale, *refs):
    me = lax.axis_index("ctx")
    barrier = pltpu.get_barrier_semaphore()
    for step in range(1, n_ctx):
        pl.semaphore_signal(barrier, inc=1, device_id={"ctx": lax.rem(me + step, n_ctx)}, device_id_type=MESH)
    pl.semaphore_wait(barrier, n_ctx - 1)
    for i in range(n_ctx):
        pl.when(me == i)(functools.partial(device_program, i, n_batch, scale, refs))


def put(*refs):
    results, outs, sem = refs[:4], refs[4:8], refs[8]
    copies = []
    for i, (result, out) in enumerate(zip(results, outs)):
        n = result.shape[0] // CHUNKS
        for c in range(CHUNKS):
            part = pl.ds(c * n, n)
            copies.append(pltpu.make_async_copy(result.at[part], out.at[part], sem.at[i, c]))
    for copy in copies:
        copy.start()
    for copy in copies:
        copy.wait()


def solution(mesh):
    part_spec = P("dp", "ctx")
    n_ctx = mesh.shape["ctx"]

    def local_step(queries, keys, values, grad_out):
        n_batch, c_len, n_q, d_head = queries.shape
        heads = (0, 2, 1, 3)
        q, do = jnp.transpose(queries, heads), jnp.transpose(grad_out, heads)
        k, v = keys.reshape(n_batch, c_len, d_head), values.reshape(n_batch, c_len, d_head)
        width = n_ctx * c_len
        vmem, dma = pltpu.VMEM, pltpu.SemaphoreType.DMA
        scratch = [
            vmem((2, n_batch, width, d_head), BF16),
            vmem((n_batch + 1, 2, c_len, d_head), F32),
            vmem((RING, 2, width - c_len, d_head), F32),
            vmem((n_batch, 2, c_len, d_head), F32),
            vmem((n_batch, 2, c_len, d_head), F32),
        ]
        scratch += [vmem((3, n_q, c_len, d_head), BF16)] * 2
        scratch += [vmem((width, 256), F32)] * 7 + [vmem((width, 256), BF16)] * 5
        scratch += [vmem((2, 8, 256), F32), vmem((3, 8, 256), F32), vmem((2, 8, 256), F32)] + [vmem((2, d_head, width), BF16)] * 2
        scratch += [dma((2,)), dma((2, n_ctx, n_batch)), dma((3, 2)), dma((n_batch,)), dma((n_batch,))] + [dma((RING,))] * 3
        scratch += [dma((3,))] * 2
        hbm = pl.BlockSpec(memory_space=pl.ANY)
        local = pl.BlockSpec(memory_space=pltpu.VMEM)
        results = pl.pallas_call(
            functools.partial(kernel, n_ctx, n_batch, d_head ** -0.5),
            out_shape=[pltpu.VMEM(x.shape, BF16) for x in (q, q, k, v)],
            in_specs=[hbm] * 4,
            out_specs=[local] * 4,
            scratch_shapes=scratch,
            compiler_params=pltpu.CompilerParams(collective_id=0, has_side_effects=True, vmem_limit_bytes=35 * 2 ** 20),
        )(q, do, k, v)
        out, grad_q, grad_k, grad_v = pl.pallas_call(
            put,
            out_shape=[jax.ShapeDtypeStruct(x.shape, BF16) for x in (q, q, k, v)],
            in_specs=[local] * 4,
            out_specs=[hbm] * 4,
            scratch_shapes=[dma((4, CHUNKS))],
            compiler_params=pltpu.CompilerParams(vmem_limit_bytes=2 ** 20),
        )(*results)
        return jnp.transpose(out, heads), jnp.transpose(grad_q, heads), grad_k.reshape(keys.shape), grad_v.reshape(values.shape)

    return jax.shard_map(local_step, mesh=mesh, in_specs=(part_spec,) * 4, out_specs=(part_spec,) * 4, check_vma=False)
```

```python
import functools

import jax
import jax.numpy as jnp
from jax import lax
from jax.experimental import pallas as pl
from jax.experimental.pallas import tpu as pltpu
from jax.sharding import PartitionSpec as P

F32, BF16 = jnp.float32, jnp.bfloat16
LOG2E = 1.4426950408889634
NEG_BIG = -1e30
MESH = pl.DeviceIdType.MESH
RING = 8
CHUNKS = 4
FLIP_AT = 1
TAIL = 3
PIECE = 32


def dot(a, b):
    return lax.dot_general(a, b, (((1,), (0,)), ((), ())), preferred_element_type=F32)


def remote(src, dst, send_sem, recv_sem, to):
    return pltpu.make_async_remote_copy(src_ref=src, dst_ref=dst, send_sem=send_sem, recv_sem=recv_sem, device_id={"ctx": to}, device_id_type=MESH)


def device_program(me, n_batch, scale, refs):
    (q_hbm, do_hbm, k_hbm, v_hbm, o_out, dq_out, dk_out, dv_out, tail_send, tail_own,
     kv, own_acc, ring, part_a, part_b, q_buf, do_buf,
     s_0, s_1, p_0, p_1, p_2, dp_0, dp_1, ph_0, ph_1, ds_0, ds_1, pb_buf, max_s, inv_s, delta_s, kt, vt,
     own_sem, kv_sem, kv_send, pa_sem, pb_sem, pa_send, pb_send, red_send,
     q_sem, do_sem) = refs
    blocks = me + 1
    width = blocks * 128
    s_buf, p_buf, dp_buf, ph_buf, ds_buf = (s_0, s_1), (p_0, p_1, p_2), (dp_0, dp_1), (ph_0, ph_1), (ds_0, ds_1)
    own = pl.ds(me * 128, 128)

    def rows(j):
        return pl.ds(j * 128, 128)

    def own_copy(a, src):
        return pltpu.make_async_copy(src, kv.at[a, :, own], own_sem.at[a])

    def kv_push(a, src, j, b, to, slot):
        return remote(src, kv.at[a, b, rows(j)], kv_send.at[slot, a], kv_sem.at[a, j, b], to)

    def kv_wait(j, b):
        for a in range(2):
            kv_push(a, kv.at[a, b, rows(j)], j, b, me, 0).wait_recv()

    def q_copy(b, slot):
        return pltpu.make_async_copy(q_hbm.at[b], q_buf.at[slot], q_sem.at[slot])

    def do_copy(b, slot):
        return pltpu.make_async_copy(do_hbm.at[b], do_buf.at[slot], do_sem.at[slot])

    def part_push(j, b, dst, send_sem, recv_sem, to):
        slot = lax.rem(b, RING) if not isinstance(b, int) else b % RING
        return remote(ring.at[slot, :, rows(j)], dst.at[b], send_sem.at[slot], recv_sem.at[b], to)

    first_hop = {0: [], 1: [(0, part_a, pa_send, pa_sem, 0)], 2: [(1, part_a, pa_send, pa_sem, 3)], 3: [(0, part_a, pa_send, pa_sem, 2), (2, part_b, pb_send, pb_sem, 2)]}[me]
    second_hop = {0: None, 1: None, 2: (0, 0), 3: (1, 1)}[me]
    relay = {0: None, 1: None, 2: (0, 3), 3: (1, 2)}[me]

    def relay_block(b):
        j, to = relay
        kv_wait(j, b)
        for a in range(2):
            kv_push(a, kv.at[a, b, rows(j)], j, b, to, 1).start()

    def kv_others(b):
        for j in range(me):
            if relay is None or j != relay[0]:
                kv_wait(j, b)

    q_copy(0, 0).start()
    do_copy(0, 0).start()
    own_copy(0, k_hbm).start()
    own_copy(1, v_hbm).start()
    direct = {0: (2, 1), 1: (3,), 2: (3,), 3: ()}[me]
    if direct:

        def push_own(b, carry):
            for slot, to in enumerate(direct):
                for a, src in enumerate((k_hbm, v_hbm)):
                    kv_push(a, src.at[b], me, b, to, 2 * slot).start()
            return carry

        lax.fori_loop(0, n_batch, push_own, 0)
    own_copy(0, k_hbm).wait()
    own_copy(1, v_hbm).wait()
    if relay is not None:
        relay_block(0)

    causal_r = lax.broadcasted_iota(jnp.int32, (128, 256), 0)
    causal_c = lax.broadcasted_iota(jnp.int32, (128, 256), 1) & 127

    def pair(ref, slot, x):
        return ref[slot, 2 * x:2 * x + 2].reshape(256, 128)

    def sub_step(x, stages, ahead=None):
        par = [(x - k) % 2 for k in range(5)]
        tri = [(x - k) % 3 for k in range(5)]
        s0, s1, s2, s3, s4 = stages
        if s0 is not None:
            qt0 = pair(q_buf, s0[3], s0[5]).T
        if s2 is not None:
            dot2 = pair(do_buf, s2[3], s2[5]).T
        if s1 is not None:
            max1 = max_s[par[1], 0:1]
        if s3 is not None:
            q3, do3 = pair(q_buf, s3[3], s3[5]), pair(do_buf, s3[3], s3[5])
            inv3, delta3 = inv_s[tri[3], 0:1], delta_s[par[3], 0:1]
        max8 = sum8 = None
        for j in range(blocks):
            r = slice(j * 128, j * 128 + 128)
            pieces = [slice(y, y + PIECE) for y in range(j * 128, j * 128 + 128, PIECE)]
            if j == 0 and s2 is not None:
                ot = (dot(vt[s2[4], :, :width], ph_buf[par[2]][:width]) * inv_s[tri[2], 0:1]).astype(BF16)
                o_out[s2[0], 2 * s2[5]:2 * s2[5] + 2] = ot.T.reshape(2, 128, 128)
                delta_s[par[2], 0:1] = jnp.sum(dot2.astype(F32) * ot.astype(F32), axis=0, keepdims=True)
            if j == min(1, blocks - 1) and s4 is not None:
                dq = (dot(kt[s4[4], :, :width], ds_buf[par[4]][:width]) * scale).astype(BF16)
                dq_out[s4[0], 2 * s4[5]:2 * s4[5] + 2] = dq.T.reshape(2, 128, 128)
            if s3 is not None:
                for y in pieces:
                    pb = p_buf[tri[3]][y] * inv3
                    ds_buf[par[3]][y] = (pb * (dp_buf[par[3]][y] - delta3)).astype(BF16)
                    pb_buf[y] = pb.astype(BF16)
                dv = dot(pb_buf[r], do3)
                dk = dot(ds_buf[par[3]][r], q3)
                for w, part in enumerate((dk, dv)):
                    dst, at = (own_acc, (s3[1], w)) if j == me else (ring, (s3[2], w, r))
                    dst[at] = part if s3[5] == 0 else dst[at] + part
            if s0 is not None:
                st = dot(kv[0, s0[0], r], qt0)
                if j == blocks - 1:
                    st = jnp.where(causal_r <= causal_c, st, NEG_BIG)
                s_buf[par[0]][r] = st
                part = jnp.max(st.reshape(16, 8, 256), axis=0)
                max8 = part if max8 is None else jnp.maximum(max8, part)
            if s1 is not None:
                for y in pieces:
                    p = jnp.exp2((s_buf[par[1]][y] - max1) * (scale * LOG2E))
                    p_buf[tri[1]][y] = p
                    ph_buf[par[1]][y] = p.astype(BF16)
                    part = jnp.sum(p.reshape(PIECE // 8, 8, 256), axis=0)
                    sum8 = part if sum8 is None else sum8 + part
            if s2 is not None:
                dp_buf[par[2]][r] = dot(kv[1, s2[0], r], dot2)
            if ahead is not None:
                kt[ahead[1], :, r] = kv[0, ahead[0], r].T
                vt[ahead[1], :, r] = kv[1, ahead[0], r].T
        if s1 is not None:
            inv_s[tri[1], 0:1] = 1.0 / jnp.sum(sum8, axis=0, keepdims=True)
        if s0 is not None:
            max_s[par[0], 0:1] = jnp.max(max8, axis=0, keepdims=True)

    def reduce_part(b):
        j, _ = second_hop
        part_push(j, b, part_a, pa_send, pa_sem, me).wait_recv()
        slot = lax.rem(b, RING) if not isinstance(b, int) else b % RING
        ring[slot, :, rows(j)] += part_a[b]

    def send_reduced(b):
        j, to = second_hop
        part_push(j, b, part_b, red_send, pb_sem, to).start()

    def send_parts(b):
        for j, dst, send_sem, recv_sem, to in first_hop:
            part_push(j, b, dst, send_sem, recv_sem, to).start()

    def sent(b):
        for j, dst, send_sem, recv_sem, to in first_hop:
            part_push(j, b, dst, send_sem, recv_sem, to).wait_send()
        if second_hop is not None and (not isinstance(b, int) or b < remote_rows):
            part_push(second_hop[0], b, part_b, red_send, pb_sem, second_hop[1]).wait_send()

    lag = 1 if me == 3 else 3
    remote_rows = n_batch - TAIL

    def step(b, carry):
        cur, prev = lax.rem(b, 3), lax.rem(b + 2, 3)
        b_prev = jnp.maximum(b - 1, 0)
        own_prev = jnp.where(b == 0, n_batch, b - 1)
        ring_cur, ring_prev = lax.rem(b, RING), lax.rem(b + RING - 1, RING)

        @pl.when(b + 1 < n_batch)
        def _():
            nxt = lax.rem(b + 1, 3)
            q_copy(b + 1, nxt).start()
            do_copy(b + 1, nxt).start()

        if me > 0:
            pl.when(b >= RING)(lambda: sent(b - RING))

        if relay is not None:

            pl.when(b + 1 < n_batch)(lambda: relay_block(b + 1))
        kv_others(b)
        q_copy(b, cur).wait()
        do_copy(b, cur).wait()
        for x in range(6):
            here = (b, b, ring_cur, cur, cur)
            before = (b_prev, own_prev, ring_prev, prev, prev)
            sub_step(x, [here + (x - k,) if x >= k else before + (x - k + 6,) for k in range(5)], (b, cur) if x == FLIP_AT else None)
        pl.when(b >= 1)(lambda: send_parts(b - 1))
        if second_hop is not None:
            pl.when(b >= lag)(lambda: reduce_part(b - lag))

        if second_hop is not None:
            pl.when((b >= lag) & (b - lag < remote_rows))(lambda: send_reduced(b - lag))
        return carry

    lax.fori_loop(0, n_batch, step, 0)

    last = n_batch - 1
    ls = last % 3
    end = (last, last, last % RING, ls, ls)
    for x in range(3):
        sub_step(x, [end + (x - k + 6,) if k > x else None for k in range(5)])
    send_parts(last)
    if me == 3:
        reduce_part(last)
    sub_step(3, [None, None, None, None, end + (5,)])
    if me == 2:
        for b in range(n_batch - lag, n_batch):
            reduce_part(b)
            if b < remote_rows:
                send_reduced(b)

    def local_sum(b):
        total = own_acc[b]
        if me == 0:
            part_push(0, b, part_a, pa_send, pa_sem, me).wait_recv()
            total = total + part_a[b]
        if me == 2:
            part_push(0, b, part_b, pb_send, pb_sem, me).wait_recv()
            total = total + part_b[b]
        return total

    def finalize(b, carry):
        total = local_sum(b)
        if me < 2:
            part_push(0, b, part_b, pb_send, pb_sem, me).wait_recv()
            total = total + part_b[b]
        dk_out[b] = (total[0] * scale).astype(BF16)
        dv_out[b] = total[1].astype(BF16)
        return carry

    for t in range(TAIL):
        b = remote_rows + t
        tail_own[t] = local_sum(b)
        tail_send[t] = jnp.zeros((2, 128, 128), F32) if second_hop is None else ring[b % RING, :, rows(second_hop[0])]
    lax.fori_loop(0, remote_rows, finalize, 0)

    if me > 0:
        for b in range(n_batch - RING, n_batch):
            sent(b)
    for slot in range(len(direct)):
        for a, src in enumerate((k_hbm, v_hbm)):
            remote(src, kv.at[a, :, own], kv_send.at[2 * slot, a], kv_sem.at[a, 0, 0], me).wait_send()
    if relay is not None:
        for a in range(2):
            remote(kv.at[a, :, rows(relay[0])], kv.at[a, :, own], kv_send.at[1, a], kv_sem.at[a, 0, 0], me).wait_send()


def kernel(n_ctx, n_batch, scale, *refs):
    me = lax.axis_index("ctx")
    barrier = pltpu.get_barrier_semaphore()
    for step in range(1, n_ctx):
        pl.semaphore_signal(barrier, inc=1, device_id={"ctx": lax.rem(me + step, n_ctx)}, device_id_type=MESH)
    pl.semaphore_wait(barrier, n_ctx - 1)
    for i in range(n_ctx):
        pl.when(me == i)(functools.partial(device_program, i, n_batch, scale, refs))


def put(*refs):
    results, outs, sem = refs[:2], refs[2:4], refs[4]
    copies = []
    for i, (result, out) in enumerate(zip(results, outs)):
        n = result.shape[0] // CHUNKS
        for c in range(CHUNKS):
            part = pl.ds(c * n, n)
            copies.append(pltpu.make_async_copy(result.at[part], out.at[part], sem.at[i, c]))
    for copy in copies:
        copy.start()
    for copy in copies:
        copy.wait()


def put_last(scale, dk_main, dv_main, own, received, dk_hbm, dv_hbm, dk_tail, dv_tail, sem):
    n = dk_main.shape[0] - TAIL
    main, tail = pl.ds(0, n), pl.ds(n, TAIL)
    copies = [pltpu.make_async_copy(dk_main.at[main], dk_hbm.at[main], sem.at[0]), pltpu.make_async_copy(dv_main.at[main], dv_hbm.at[main], sem.at[1])]
    for copy in copies:
        copy.start()
    total = own[...] + received[...]
    dk_tail[...] = (total[:, 0] * scale).astype(BF16)
    dv_tail[...] = total[:, 1].astype(BF16)
    last = [pltpu.make_async_copy(dk_tail, dk_hbm.at[tail], sem.at[2]), pltpu.make_async_copy(dv_tail, dv_hbm.at[tail], sem.at[3])]
    for copy in last:
        copy.start()
    for copy in copies + last:
        copy.wait()


def solution(mesh):
    part_spec = P("dp", "ctx")
    n_ctx = mesh.shape["ctx"]

    def local_step(queries, keys, values, grad_out):
        n_batch, c_len, n_q, d_head = queries.shape
        heads = (0, 2, 1, 3)
        q, do = jnp.transpose(queries, heads), jnp.transpose(grad_out, heads)
        k, v = keys.reshape(n_batch, c_len, d_head), values.reshape(n_batch, c_len, d_head)
        width = n_ctx * c_len
        vmem, dma = pltpu.VMEM, pltpu.SemaphoreType.DMA
        scratch = [
            vmem((2, n_batch, width, d_head), BF16),
            vmem((n_batch + 1, 2, c_len, d_head), F32),
            vmem((RING, 2, width - c_len, d_head), F32),
            vmem((n_batch, 2, c_len, d_head), F32),
            vmem((n_batch, 2, c_len, d_head), F32),
        ]
        scratch += [vmem((3, n_q, c_len, d_head), BF16)] * 2
        scratch += [vmem((width, 256), F32)] * 7 + [vmem((width, 256), BF16)] * 5
        scratch += [vmem((2, 8, 256), F32), vmem((3, 8, 256), F32), vmem((2, 8, 256), F32)] + [vmem((3, d_head, width), BF16)] * 2
        scratch += [dma((2,)), dma((2, n_ctx, n_batch)), dma((3, 2)), dma((n_batch,)), dma((n_batch,))] + [dma((RING,))] * 3
        scratch += [dma((3,))] * 2
        hbm = pl.BlockSpec(memory_space=pl.ANY)
        local = pl.BlockSpec(memory_space=pltpu.VMEM)
        scale = d_head ** -0.5
        tail = (TAIL, 2, c_len, d_head)
        out, grad_q, grad_k, grad_v, tail_send, tail_own = pl.pallas_call(
            functools.partial(kernel, n_ctx, n_batch, scale),
            out_shape=[pltpu.VMEM(x.shape, BF16) for x in (q, q, k, v)] + [pltpu.VMEM(tail, F32), pltpu.VMEM(tail, F32)],
            in_specs=[hbm] * 4,
            out_specs=[local] * 6,
            scratch_shapes=scratch,
            compiler_params=pltpu.CompilerParams(collective_id=0, has_side_effects=True, vmem_limit_bytes=35 * 2 ** 20),
        )(q, do, k, v)
        received = lax.ppermute(tail_send, "ctx", [(2, 0), (3, 1)])
        out, grad_q = pl.pallas_call(
            put,
            out_shape=[jax.ShapeDtypeStruct(q.shape, BF16)] * 2,
            in_specs=[local] * 2,
            out_specs=[hbm] * 2,
            scratch_shapes=[dma((2, CHUNKS))],
            cost_estimate=pl.CostEstimate(flops=10 ** 10, bytes_accessed=2 * q.size * 2, transcendentals=0),
            compiler_params=pltpu.CompilerParams(vmem_limit_bytes=2 ** 20),
        )(out, grad_q)
        grad_k, grad_v = pl.pallas_call(
            functools.partial(put_last, scale),
            out_shape=[jax.ShapeDtypeStruct(k.shape, BF16)] * 2,
            in_specs=[local] * 4,
            out_specs=[hbm] * 2,
            scratch_shapes=[vmem((TAIL, c_len, d_head), BF16)] * 2 + [dma((4,))],
            compiler_params=pltpu.CompilerParams(vmem_limit_bytes=4 * 2 ** 20),
        )(grad_k, grad_v, tail_own, received)
        return jnp.transpose(out, heads), jnp.transpose(grad_q, heads), grad_k.reshape(keys.shape), grad_v.reshape(values.shape)

    return jax.shard_map(local_step, mesh=mesh, in_specs=(part_spec,) * 4, out_specs=(part_spec,) * 4, check_vma=False)
```

```python
import functools

import jax
import jax.numpy as jnp
from jax import lax
from jax.experimental import pallas as pl
from jax.experimental.pallas import tpu as pltpu
from jax.sharding import PartitionSpec as P

F32, BF16 = jnp.float32, jnp.bfloat16
LOG2E = 1.4426950408889634
NEG_BIG = -1e30
MESH = pl.DeviceIdType.MESH
RING = 8
CHUNKS = 4
FLIP_AT = 1
TAIL = 2
PIECE = 32


def dot(a, b):
    return lax.dot_general(a, b, (((1,), (0,)), ((), ())), preferred_element_type=F32)


def remote(src, dst, send_sem, recv_sem, to):
    return pltpu.make_async_remote_copy(src_ref=src, dst_ref=dst, send_sem=send_sem, recv_sem=recv_sem, device_id={"ctx": to}, device_id_type=MESH)


def device_program(me, n_batch, scale, refs):
    (q_hbm, do_hbm, k_hbm, v_hbm, o_out, dq_out, dk_out, dv_out, tail_send, tail_own,
     kv, own_acc, ring, part_a, part_b, q_buf, do_buf,
     s_0, s_1, p_0, p_1, p_2, dp_0, dp_1, ph_0, ph_1, ds_0, ds_1, pb_buf, max_s, inv_s, delta_s, kt, vt,
     own_sem, kv_sem, kv_send, pa_sem, pb_sem, pa_send, pb_send, red_send,
     q_sem, do_sem) = refs
    blocks = me + 1
    width = blocks * 128
    s_buf, p_buf, dp_buf, ph_buf, ds_buf = (s_0, s_1), (p_0, p_1, p_2), (dp_0, dp_1), (ph_0, ph_1), (ds_0, ds_1)
    own = pl.ds(me * 128, 128)

    def rows(j):
        return pl.ds(j * 128, 128)

    def own_copy(a, src):
        return pltpu.make_async_copy(src, kv.at[a, :, own], own_sem.at[a])

    def kv_push(a, src, j, b, to, slot):
        return remote(src, kv.at[a, b, rows(j)], kv_send.at[slot, a], kv_sem.at[a, j, b], to)

    def kv_wait(j, b):
        for a in range(2):
            kv_push(a, kv.at[a, b, rows(j)], j, b, me, 0).wait_recv()

    def q_copy(b, slot):
        return pltpu.make_async_copy(q_hbm.at[b], q_buf.at[slot], q_sem.at[slot])

    def do_copy(b, slot):
        return pltpu.make_async_copy(do_hbm.at[b], do_buf.at[slot], do_sem.at[slot])

    def part_push(j, b, dst, send_sem, recv_sem, to):
        slot = lax.rem(b, RING) if not isinstance(b, int) else b % RING
        return remote(ring.at[slot, :, rows(j)], dst.at[b], send_sem.at[slot], recv_sem.at[b], to)

    first_hop = {0: [], 1: [(0, part_a, pa_send, pa_sem, 0)], 2: [(1, part_a, pa_send, pa_sem, 3)], 3: [(0, part_a, pa_send, pa_sem, 2), (2, part_b, pb_send, pb_sem, 2)]}[me]
    second_hop = {0: None, 1: None, 2: (0, 0), 3: (1, 1)}[me]
    relay = {0: None, 1: None, 2: (0, 3), 3: (1, 2)}[me]

    def relay_block(b):
        j, to = relay
        kv_wait(j, b)
        for a in range(2):
            kv_push(a, kv.at[a, b, rows(j)], j, b, to, 1).start()

    def kv_others(b):
        for j in range(me):
            if relay is None or j != relay[0]:
                kv_wait(j, b)

    direct = {0: (2, 1), 1: (3,), 2: (3,), 3: ()}[me]

    def push_own(b, carry):
        for slot, to in enumerate(direct):
            for a, src in enumerate((k_hbm, v_hbm)):
                kv_push(a, src.at[b], me, b, to, 2 * slot).start()
        return carry

    push_own(0, 0)
    own_copy(0, k_hbm).start()
    own_copy(1, v_hbm).start()
    q_copy(0, 0).start()
    do_copy(0, 0).start()
    if direct:
        lax.fori_loop(1, n_batch, push_own, 0)
    own_copy(0, k_hbm).wait()
    own_copy(1, v_hbm).wait()
    if relay is not None:
        relay_block(0)

    causal_r = lax.broadcasted_iota(jnp.int32, (128, 256), 0)
    causal_c = lax.broadcasted_iota(jnp.int32, (128, 256), 1) & 127

    def pair(ref, slot, x):
        return ref[slot, 2 * x:2 * x + 2].reshape(256, 128)

    def sub_step(x, stages, ahead=None):
        par = [(x - k) % 2 for k in range(5)]
        tri = [(x - k) % 3 for k in range(5)]
        s0, s1, s2, s3, s4 = stages
        if s0 is not None:
            qt0 = pair(q_buf, s0[3], s0[5]).T
        if s2 is not None:
            dot2 = pair(do_buf, s2[3], s2[5]).T
        if s1 is not None:
            max1 = max_s[par[1], 0:1]
        if s3 is not None:
            q3, do3 = pair(q_buf, s3[3], s3[5]), pair(do_buf, s3[3], s3[5])
            inv3, delta3 = inv_s[tri[3], 0:1], delta_s[par[3], 0:1]
        max8 = sum8 = None
        for j in range(blocks):
            r = slice(j * 128, j * 128 + 128)
            pieces = [slice(y, y + PIECE) for y in range(j * 128, j * 128 + 128, PIECE)]
            if j == 0 and s2 is not None:
                ot = (dot(vt[s2[4], :, :width], ph_buf[par[2]][:width]) * inv_s[tri[2], 0:1]).astype(BF16)
                o_out[s2[0], 2 * s2[5]:2 * s2[5] + 2] = ot.T.reshape(2, 128, 128)
                delta_s[par[2], 0:1] = jnp.sum(dot2.astype(F32) * ot.astype(F32), axis=0, keepdims=True)
            if j == min(1, blocks - 1) and s4 is not None:
                dq = (dot(kt[s4[4], :, :width], ds_buf[par[4]][:width]) * scale).astype(BF16)
                dq_out[s4[0], 2 * s4[5]:2 * s4[5] + 2] = dq.T.reshape(2, 128, 128)
            if s3 is not None:
                for y in pieces:
                    pb = p_buf[tri[3]][y] * inv3
                    ds_buf[par[3]][y] = (pb * (dp_buf[par[3]][y] - delta3)).astype(BF16)
                    pb_buf[y] = pb.astype(BF16)
                dv = dot(pb_buf[r], do3)
                dk = dot(ds_buf[par[3]][r], q3)
                for w, part in enumerate((dk, dv)):
                    dst, at = (own_acc, (s3[1], w)) if j == me else (ring, (s3[2], w, r))
                    dst[at] = part if s3[5] == 0 else dst[at] + part
            if s0 is not None:
                st = dot(kv[0, s0[0], r], qt0)
                if j == blocks - 1:
                    st = jnp.where(causal_r <= causal_c, st, NEG_BIG)
                s_buf[par[0]][r] = st
                part = jnp.max(st.reshape(16, 8, 256), axis=0)
                max8 = part if max8 is None else jnp.maximum(max8, part)
            if s1 is not None:
                for y in pieces:
                    p = jnp.exp2((s_buf[par[1]][y] - max1) * (scale * LOG2E))
                    p_buf[tri[1]][y] = p
                    ph_buf[par[1]][y] = p.astype(BF16)
                    part = jnp.sum(p.reshape(PIECE // 8, 8, 256), axis=0)
                    sum8 = part if sum8 is None else sum8 + part
            if s2 is not None:
                dp_buf[par[2]][r] = dot(kv[1, s2[0], r], dot2)
            if ahead is not None:
                kt[ahead[1], :, r] = kv[0, ahead[0], r].T
                vt[ahead[1], :, r] = kv[1, ahead[0], r].T
        if s1 is not None:
            inv_s[tri[1], 0:1] = 1.0 / jnp.sum(sum8, axis=0, keepdims=True)
        if s0 is not None:
            max_s[par[0], 0:1] = jnp.max(max8, axis=0, keepdims=True)

    def reduce_part(b):
        j, _ = second_hop
        part_push(j, b, part_a, pa_send, pa_sem, me).wait_recv()
        slot = lax.rem(b, RING) if not isinstance(b, int) else b % RING
        ring[slot, :, rows(j)] += part_a[b]

    def send_reduced(b):
        j, to = second_hop
        part_push(j, b, part_b, red_send, pb_sem, to).start()

    def send_parts(b):
        for j, dst, send_sem, recv_sem, to in first_hop:
            part_push(j, b, dst, send_sem, recv_sem, to).start()

    def sent(b):
        for j, dst, send_sem, recv_sem, to in first_hop:
            part_push(j, b, dst, send_sem, recv_sem, to).wait_send()
        if second_hop is not None and (not isinstance(b, int) or b < remote_rows):
            part_push(second_hop[0], b, part_b, red_send, pb_sem, second_hop[1]).wait_send()

    lag = 1 if me == 3 else 2
    remote_rows = n_batch - TAIL

    def step(b, carry):
        cur, prev = lax.rem(b, 3), lax.rem(b + 2, 3)
        b_prev = jnp.maximum(b - 1, 0)
        own_prev = jnp.where(b == 0, n_batch, b - 1)
        ring_cur, ring_prev = lax.rem(b, RING), lax.rem(b + RING - 1, RING)

        @pl.when(b + 1 < n_batch)
        def _():
            nxt = lax.rem(b + 1, 3)
            q_copy(b + 1, nxt).start()
            do_copy(b + 1, nxt).start()

        if me > 0:
            pl.when(b >= RING)(lambda: sent(b - RING))

        if relay is not None:

            pl.when(b + 1 < n_batch)(lambda: relay_block(b + 1))
        kv_others(b)
        q_copy(b, cur).wait()
        do_copy(b, cur).wait()
        for x in range(6):
            here = (b, b, ring_cur, cur, cur)
            before = (b_prev, own_prev, ring_prev, prev, prev)
            sub_step(x, [here + (x - k,) if x >= k else before + (x - k + 6,) for k in range(5)], (b, cur) if x == FLIP_AT else None)
        pl.when(b >= 1)(lambda: send_parts(b - 1))
        if second_hop is not None:
            pl.when(b >= lag)(lambda: reduce_part(b - lag))

        if second_hop is not None:
            pl.when((b >= lag) & (b - lag < remote_rows))(lambda: send_reduced(b - lag))
        return carry

    lax.fori_loop(0, n_batch, step, 0)

    last = n_batch - 1
    ls = last % 3
    end = (last, last, last % RING, ls, ls)
    for x in range(3):
        sub_step(x, [end + (x - k + 6,) if k > x else None for k in range(5)])
    send_parts(last)
    if me == 3:
        reduce_part(last)
    sub_step(3, [None, None, None, None, end + (5,)])
    if me == 2:
        for b in range(n_batch - lag, n_batch):
            reduce_part(b)
            if b < remote_rows:
                send_reduced(b)

    def local_sum(b):
        total = own_acc[b]
        if me == 0:
            part_push(0, b, part_a, pa_send, pa_sem, me).wait_recv()
            total = total + part_a[b]
        if me == 2:
            part_push(0, b, part_b, pb_send, pb_sem, me).wait_recv()
            total = total + part_b[b]
        return total

    def finalize(b, carry):
        total = local_sum(b)
        if me < 2:
            part_push(0, b, part_b, pb_send, pb_sem, me).wait_recv()
            total = total + part_b[b]
        dk_out[b] = (total[0] * scale).astype(BF16)
        dv_out[b] = total[1].astype(BF16)
        return carry

    for t in range(TAIL):
        b = remote_rows + t
        tail_own[t] = local_sum(b)
        tail_send[t] = jnp.zeros((2, 128, 128), F32) if second_hop is None else ring[b % RING, :, rows(second_hop[0])]
    lax.fori_loop(0, remote_rows, finalize, 0)

    if me > 0:
        for b in range(n_batch - RING, n_batch):
            sent(b)
    for slot in range(len(direct)):
        for a, src in enumerate((k_hbm, v_hbm)):
            remote(src, kv.at[a, :, own], kv_send.at[2 * slot, a], kv_sem.at[a, 0, 0], me).wait_send()
    if relay is not None:
        for a in range(2):
            remote(kv.at[a, :, rows(relay[0])], kv.at[a, :, own], kv_send.at[1, a], kv_sem.at[a, 0, 0], me).wait_send()


def kernel(n_ctx, n_batch, scale, *refs):
    me = lax.axis_index("ctx")
    barrier = pltpu.get_barrier_semaphore()
    for step in range(1, n_ctx):
        pl.semaphore_signal(barrier, inc=1, device_id={"ctx": lax.rem(me + step, n_ctx)}, device_id_type=MESH)
    pl.semaphore_wait(barrier, n_ctx - 1)
    for i in range(n_ctx):
        pl.when(me == i)(functools.partial(device_program, i, n_batch, scale, refs))


def put(*refs):
    results, outs, sem = refs[:2], refs[2:4], refs[4]
    copies = []
    for i, (result, out) in enumerate(zip(results, outs)):
        n = result.shape[0] // CHUNKS
        for c in range(CHUNKS):
            part = pl.ds(c * n, n)
            copies.append(pltpu.make_async_copy(result.at[part], out.at[part], sem.at[i, c]))
    for copy in copies:
        copy.start()
    for copy in copies:
        copy.wait()


def put_last(scale, dk_main, dv_main, own, received, dk_hbm, dv_hbm, dk_tail, dv_tail, sem):
    n = dk_main.shape[0] - TAIL
    main, tail = pl.ds(0, n), pl.ds(n, TAIL)
    copies = [pltpu.make_async_copy(dk_main.at[main], dk_hbm.at[main], sem.at[0]), pltpu.make_async_copy(dv_main.at[main], dv_hbm.at[main], sem.at[1])]
    for copy in copies:
        copy.start()
    total = own[...] + received[...]
    dk_tail[...] = (total[:, 0] * scale).astype(BF16)
    dv_tail[...] = total[:, 1].astype(BF16)
    last = [pltpu.make_async_copy(dk_tail, dk_hbm.at[tail], sem.at[2]), pltpu.make_async_copy(dv_tail, dv_hbm.at[tail], sem.at[3])]
    for copy in last:
        copy.start()
    for copy in copies + last:
        copy.wait()


def solution(mesh):
    part_spec = P("dp", "ctx")
    n_ctx = mesh.shape["ctx"]

    def local_step(queries, keys, values, grad_out):
        n_batch, c_len, n_q, d_head = queries.shape
        heads = (0, 2, 1, 3)
        q, do = jnp.transpose(queries, heads), jnp.transpose(grad_out, heads)
        k, v = keys.reshape(n_batch, c_len, d_head), values.reshape(n_batch, c_len, d_head)
        width = n_ctx * c_len
        vmem, dma = pltpu.VMEM, pltpu.SemaphoreType.DMA
        scratch = [
            vmem((2, n_batch, width, d_head), BF16),
            vmem((n_batch + 1, 2, c_len, d_head), F32),
            vmem((RING, 2, width - c_len, d_head), F32),
            vmem((n_batch, 2, c_len, d_head), F32),
            vmem((n_batch, 2, c_len, d_head), F32),
        ]
        scratch += [vmem((3, n_q, c_len, d_head), BF16)] * 2
        scratch += [vmem((width, 256), F32)] * 7 + [vmem((width, 256), BF16)] * 5
        scratch += [vmem((2, 8, 256), F32), vmem((3, 8, 256), F32), vmem((2, 8, 256), F32)] + [vmem((3, d_head, width), BF16)] * 2
        scratch += [dma((2,)), dma((2, n_ctx, n_batch)), dma((3, 2)), dma((n_batch,)), dma((n_batch,))] + [dma((RING,))] * 3
        scratch += [dma((3,))] * 2
        hbm = pl.BlockSpec(memory_space=pl.ANY)
        local = pl.BlockSpec(memory_space=pltpu.VMEM)
        scale = d_head ** -0.5
        tail = (TAIL, 2, c_len, d_head)
        out, grad_q, grad_k, grad_v, tail_send, tail_own = pl.pallas_call(
            functools.partial(kernel, n_ctx, n_batch, scale),
            out_shape=[pltpu.VMEM(x.shape, BF16) for x in (q, q, k, v)] + [pltpu.VMEM(tail, F32), pltpu.VMEM(tail, F32)],
            in_specs=[hbm] * 4,
            out_specs=[local] * 6,
            scratch_shapes=scratch,
            compiler_params=pltpu.CompilerParams(collective_id=0, has_side_effects=True, vmem_limit_bytes=35 * 2 ** 20),
        )(q, do, k, v)
        received = lax.ppermute(tail_send, "ctx", [(2, 0), (3, 1)])
        out, grad_q = pl.pallas_call(
            put,
            out_shape=[jax.ShapeDtypeStruct(q.shape, BF16)] * 2,
            in_specs=[local] * 2,
            out_specs=[hbm] * 2,
            scratch_shapes=[dma((2, CHUNKS))],
            cost_estimate=pl.CostEstimate(flops=10 ** 10, bytes_accessed=2 * q.size * 2, transcendentals=0),
            compiler_params=pltpu.CompilerParams(vmem_limit_bytes=2 ** 20),
        )(out, grad_q)
        grad_k, grad_v = pl.pallas_call(
            functools.partial(put_last, scale),
            out_shape=[jax.ShapeDtypeStruct(k.shape, BF16)] * 2,
            in_specs=[local] * 4,
            out_specs=[hbm] * 2,
            scratch_shapes=[vmem((TAIL, c_len, d_head), BF16)] * 2 + [dma((4,))],
            compiler_params=pltpu.CompilerParams(vmem_limit_bytes=4 * 2 ** 20),
        )(grad_k, grad_v, tail_own, received)
        return jnp.transpose(out, heads), jnp.transpose(grad_q, heads), grad_k.reshape(keys.shape), grad_v.reshape(values.shape)

    return jax.shard_map(local_step, mesh=mesh, in_specs=(part_spec,) * 4, out_specs=(part_spec,) * 4, check_vma=False)
```

```python
import functools

import jax
import jax.numpy as jnp
from jax import lax
from jax.experimental import pallas as pl
from jax.experimental.pallas import tpu as pltpu
from jax.sharding import PartitionSpec as P

F32, BF16 = jnp.float32, jnp.bfloat16
LOG2E = 1.4426950408889634
NEG_BIG = -1e30
MESH = pl.DeviceIdType.MESH
RING = 9
CHUNKS = 4
FLIP_AT = 1
TAIL = 3
PIECE = 32


def dot(a, b):
    return lax.dot_general(a, b, (((1,), (0,)), ((), ())), preferred_element_type=F32)


def remote(src, dst, send_sem, recv_sem, to):
    return pltpu.make_async_remote_copy(src_ref=src, dst_ref=dst, send_sem=send_sem, recv_sem=recv_sem, device_id={"ctx": to}, device_id_type=MESH)


def device_program(me, n_batch, scale, refs):
    (q_hbm, do_hbm, k_hbm, v_hbm, o_out, dq_out, dk_out, dv_out, tail_send, tail_own,
     kv, own_acc, ring, part_a, part_b, q_buf, do_buf,
     s_0, s_1, p_0, p_1, p_2, dp_0, dp_1, ph_0, ph_1, ds_0, ds_1, pb_buf, max_s, inv_s, delta_s, kt, vt,
     own_sem, kv_sem, kv_send, pa_sem, pb_sem, pa_send, pb_send, red_send,
     q_sem, do_sem, x_q, x_do, x_acc, x_sem, x_send, xo_sem, xo_send, xa_send) = refs
    blocks = me + 1
    remote_rows = n_batch - TAIL
    n_rows = remote_rows if me == 3 else n_batch
    s_buf, p_buf, dp_buf, ph_buf, ds_buf = (s_0, s_1), (p_0, p_1, p_2), (dp_0, dp_1), (ph_0, ph_1), (ds_0, ds_1)
    own = pl.ds(me * 128, 128)

    def rows(j):
        return pl.ds(j * 128, 128)

    def own_copy(a, src):
        return pltpu.make_async_copy(src, kv.at[a, :, own], own_sem.at[a])

    def kv_push(a, src, j, b, to, slot):
        return remote(src, kv.at[a, b, rows(j)], kv_send.at[slot, a], kv_sem.at[a, j, b], to)

    def kv_wait(j, b):
        for a in range(2):
            kv_push(a, kv.at[a, b, rows(j)], j, b, me, 0).wait_recv()

    def q_copy(b, slot):
        return pltpu.make_async_copy(q_hbm.at[b], q_buf.at[slot], q_sem.at[slot])

    def do_copy(b, slot):
        return pltpu.make_async_copy(do_hbm.at[b], do_buf.at[slot], do_sem.at[slot])

    def part_push(j, b, dst, send_sem, recv_sem, to):
        slot = lax.rem(b, RING) if not isinstance(b, int) else b % RING
        return remote(ring.at[slot, :, rows(j)], dst.at[b], send_sem.at[slot], recv_sem.at[b], to)

    first_hop = {0: [], 1: [(0, part_a, pa_send, pa_sem, 0)], 2: [(1, part_a, pa_send, pa_sem, 3)], 3: [(0, part_a, pa_send, pa_sem, 2), (2, part_b, pb_send, pb_sem, 2)]}[me]
    second_hop = {0: None, 1: None, 2: (0, 0), 3: (1, 1)}[me]
    relay = {0: None, 1: None, 2: (0, 3), 3: (1, 2)}[me]

    def relay_block(b):
        j, to = relay
        kv_wait(j, b)
        for a in range(2):
            kv_push(a, kv.at[a, b, rows(j)], j, b, to, 1).start()

    def kv_others(b):
        for j in range(me):
            if relay is None or j != relay[0]:
                kv_wait(j, b)

    def extra_in(e, to):
        b = remote_rows + e
        moves = [remote(q_hbm.at[b], x_q.at[e], x_send.at[0, e], x_sem.at[0, e], to), remote(do_hbm.at[b], x_do.at[e], x_send.at[1, e], x_sem.at[1, e], to)]
        for a, src in enumerate((k_hbm, v_hbm)):
            moves.append(remote(src.at[b], kv.at[a, b, rows(3)], x_send.at[2 + a, e], kv_sem.at[a, 3, b], to))
        return moves

    def extra_out(e, to):
        b = remote_rows + e
        return [remote(q_buf.at[e], o_out.at[b], xo_send.at[0, e], xo_sem.at[0, e], to), remote(do_buf.at[e], dq_out.at[b], xo_send.at[1, e], xo_sem.at[1, e], to)]

    def extra_acc(e, to):
        return remote(x_acc.at[e], part_b.at[remote_rows + e], xa_send.at[e], pb_sem.at[remote_rows + e], to)

    direct = {0: (2, 1), 1: (3,), 2: (3,), 3: ()}[me]

    def push_own(b, carry):
        for slot, to in enumerate(direct):
            for a, src in enumerate((k_hbm, v_hbm)):
                kv_push(a, src.at[b], me, b, to, 2 * slot).start()
        return carry

    push_own(0, 0)
    own_copy(0, k_hbm).start()
    own_copy(1, v_hbm).start()
    q_copy(0, 0).start()
    do_copy(0, 0).start()
    if direct:
        lax.fori_loop(1, n_batch, push_own, 0)
    own_copy(0, k_hbm).wait()
    own_copy(1, v_hbm).wait()
    if relay is not None:
        relay_block(0)

    causal_r = lax.broadcasted_iota(jnp.int32, (128, 256), 0)
    causal_c = lax.broadcasted_iota(jnp.int32, (128, 256), 1) & 127

    def pair(ref, slot, x):
        return ref[slot, 2 * x:2 * x + 2].reshape(256, 128)

    def main_acc(j, s3):
        return (own_acc, (s3[1],), True) if j == me else (ring, (s3[2],), True)

    def extra_row_acc(j, s3):
        if j == 3:
            return x_acc, (s3[1] - remote_rows,), True
        return (own_acc, (s3[1],), False) if j == me else (ring, (s3[2],), False)

    main_cfg = (blocks, q_buf, do_buf, o_out, dq_out, 0, main_acc)
    extra_cfg = (blocks + 1, x_q, x_do, q_buf, do_buf, 3, extra_row_acc)

    def sub_step(x, stages, ahead=None, cfg=main_cfg):
        blocks, q_src, do_src, o_dst, dq_dst, at, acc_of = cfg
        width = blocks * 128
        par = [(x - k) % 2 for k in range(5)]
        tri = [(x - k) % 3 for k in range(5)]
        s0, s1, s2, s3, s4 = stages
        if s0 is not None:
            qt0 = pair(q_src, s0[3], s0[5]).T
        if s2 is not None:
            dot2 = pair(do_src, s2[3], s2[5]).T
        if s1 is not None:
            max1 = max_s[par[1], 0:1]
        if s3 is not None:
            q3, do3 = pair(q_src, s3[3], s3[5]), pair(do_src, s3[3], s3[5])
            inv3, delta3 = inv_s[tri[3], 0:1], delta_s[par[3], 0:1]
        max8 = sum8 = None
        for j in range(blocks):
            r = slice(j * 128, j * 128 + 128)
            pieces = [slice(y, y + PIECE) for y in range(j * 128, j * 128 + 128, PIECE)]
            if j == 0 and s2 is not None:
                ot = (dot(vt[s2[4], :, :width], ph_buf[par[2]][:width]) * inv_s[tri[2], 0:1]).astype(BF16)
                o_dst[s2[at], 2 * s2[5]:2 * s2[5] + 2] = ot.T.reshape(2, 128, 128)
                delta_s[par[2], 0:1] = jnp.sum(dot2.astype(F32) * ot.astype(F32), axis=0, keepdims=True)
            if j == min(1, blocks - 1) and s4 is not None:
                dq = (dot(kt[s4[4], :, :width], ds_buf[par[4]][:width]) * scale).astype(BF16)
                dq_dst[s4[at], 2 * s4[5]:2 * s4[5] + 2] = dq.T.reshape(2, 128, 128)
            if s3 is not None:
                for y in pieces:
                    pb = p_buf[tri[3]][y] * inv3
                    ds_buf[par[3]][y] = (pb * (dp_buf[par[3]][y] - delta3)).astype(BF16)
                    pb_buf[y] = pb.astype(BF16)
                dv = dot(pb_buf[r], do3)
                dk = dot(ds_buf[par[3]][r], q3)
                dst, idx, fresh = acc_of(j, s3)
                for w, part in enumerate((dk, dv)):
                    where = idx + ((w,) if dst is not ring else (w, r))
                    dst[where] = part if fresh and s3[5] == 0 else dst[where] + part
            if s0 is not None:
                st = dot(kv[0, s0[0], r], qt0)
                if j == blocks - 1:
                    st = jnp.where(causal_r <= causal_c, st, NEG_BIG)
                s_buf[par[0]][r] = st
                part = jnp.max(st.reshape(16, 8, 256), axis=0)
                max8 = part if max8 is None else jnp.maximum(max8, part)
            if s1 is not None:
                for y in pieces:
                    p = jnp.exp2((s_buf[par[1]][y] - max1) * (scale * LOG2E))
                    p_buf[tri[1]][y] = p
                    ph_buf[par[1]][y] = p.astype(BF16)
                    part = jnp.sum(p.reshape(PIECE // 8, 8, 256), axis=0)
                    sum8 = part if sum8 is None else sum8 + part
            if s2 is not None:
                dp_buf[par[2]][r] = dot(kv[1, s2[0], r], dot2)
            if ahead is not None:
                kt[ahead[1], :, r] = kv[0, ahead[0], r].T
                vt[ahead[1], :, r] = kv[1, ahead[0], r].T
        if s1 is not None:
            inv_s[tri[1], 0:1] = 1.0 / jnp.sum(sum8, axis=0, keepdims=True)
        if s0 is not None:
            max_s[par[0], 0:1] = jnp.max(max8, axis=0, keepdims=True)

    def reduce_part(b):
        j, _ = second_hop
        part_push(j, b, part_a, pa_send, pa_sem, me).wait_recv()
        slot = lax.rem(b, RING) if not isinstance(b, int) else b % RING
        ring[slot, :, rows(j)] += part_a[b]

    def send_reduced(b):
        j, to = second_hop
        part_push(j, b, part_b, red_send, pb_sem, to).start()

    def send_parts(b):
        for j, dst, send_sem, recv_sem, to in first_hop:
            part_push(j, b, dst, send_sem, recv_sem, to).start()

    def sent(b):
        for j, dst, send_sem, recv_sem, to in first_hop:
            part_push(j, b, dst, send_sem, recv_sem, to).wait_send()
        if second_hop is not None and (not isinstance(b, int) or b < remote_rows):
            part_push(second_hop[0], b, part_b, red_send, pb_sem, second_hop[1]).wait_send()

    def paced(b):
        return jnp.maximum(b, 0) if me == 3 else jnp.maximum((82 * (b + 1) - 142) // 100, 0)


    def step(b, carry):
        cur, prev = lax.rem(b, 3), lax.rem(b + 2, 3)
        b_prev = jnp.maximum(b - 1, 0)
        own_prev = jnp.where(b == 0, n_batch, b - 1)
        ring_cur, ring_prev = lax.rem(b, RING), lax.rem(b + RING - 1, RING)

        @pl.when(b + 1 < n_rows)
        def _():
            nxt = lax.rem(b + 1, 3)
            q_copy(b + 1, nxt).start()
            do_copy(b + 1, nxt).start()

        if me > 0:
            pl.when(b >= RING)(lambda: sent(b - RING))

        if relay is not None:

            if me == 2:
                pl.when(b + 1 < n_batch)(lambda: relay_block(b + 1))
            else:
                pl.when((b >= 1) & (2 * b < n_batch))(lambda: relay_block(2 * b))
                pl.when(2 * b + 1 < n_batch)(lambda: relay_block(2 * b + 1))
        kv_others(b)
        q_copy(b, cur).wait()
        do_copy(b, cur).wait()
        for x in range(6):
            here = (b, b, ring_cur, cur, cur)
            before = (b_prev, own_prev, ring_prev, prev, prev)
            sub_step(x, [here + (x - k,) if x >= k else before + (x - k + 6,) for k in range(5)], (b, cur) if x == FLIP_AT else None)
        pl.when((b >= 1) & (b <= remote_rows) if me == 2 else b >= 1)(lambda: send_parts(b - 1))

        if second_hop is not None:

            @pl.when(paced(b) > paced(b - 1))
            def _():
                reduce_part(paced(b) - 1)
                send_reduced(paced(b) - 1)

        if me == 3:

            @pl.when(b < TAIL)
            def _():
                for move in extra_in(b, 2):
                    move.start()

        return carry

    lax.fori_loop(0, n_rows, step, 0)

    last = n_rows - 1
    ls = last % 3
    end = (last, last, last % RING, ls, ls)
    for x in range(3):
        sub_step(x, [end + (x - k + 6,) if k > x else None for k in range(5)])
    if me != 2:
        send_parts(last)
    if me == 3:
        reduce_part(last)
    sub_step(3, [None, None, None, None, end + (5,)])
    if me == 3:
        send_reduced(last)

    def reduce_and_send(b):
        reduce_part(b)
        send_reduced(b)

    if me == 2:
        for b in range((82 * n_batch - 142) // 100, remote_rows - 1 - TAIL):
            reduce_and_send(b)

        def extra(e, carry):
            b = remote_rows + e
            prev = lax.rem(e + 2, 3)
            here = (b, b, lax.rem(b, RING), e, e)
            before = (jnp.maximum(b - 1, remote_rows), jnp.where(e == 0, n_batch, b - 1), jnp.where(e == 0, RING, lax.rem(b - 1, RING)), prev, prev)
            for x in range(6):
                sub_step(x, [here + (x - k,) if x >= k else before + (x - k + 6,) for k in range(5)], (b, e) if x == FLIP_AT else None, extra_cfg)

            @pl.when(e >= 1)
            def _():
                for move in extra_out(e - 1, 3):
                    move.start()
                extra_acc(e - 1, 3).start()
                send_parts(b - 1)

            reduce_and_send(remote_rows - 1 - TAIL + e)
            return carry

        for e in range(TAIL):
            for move in extra_in(e, me):
                move.wait_recv()
        lax.fori_loop(0, TAIL, extra, 0)
        end = (n_batch - 1, n_batch - 1, (n_batch - 1) % RING, TAIL - 1, TAIL - 1)
        for x in range(3):
            sub_step(x, [end + (x - k + 6,) if k > x else None for k in range(5)], None, extra_cfg)
        extra_acc(TAIL - 1, 3).start()
        send_parts(n_batch - 1)
        sub_step(3, [None, None, None, None, end + (5,)], None, extra_cfg)
        reduce_and_send(remote_rows - 1)
        for move in extra_out(TAIL - 1, 3):
            move.start()

    def local_sum(b):
        if me == 3 and isinstance(b, int) and b >= remote_rows:
            extra_acc(b - remote_rows, me).wait_recv()
            return part_b[b]
        total = own_acc[b]
        if me == 0:
            part_push(0, b, part_a, pa_send, pa_sem, me).wait_recv()
            total = total + part_a[b]
        if me == 2 and not (isinstance(b, int) and b >= remote_rows):
            part_push(0, b, part_b, pb_send, pb_sem, me).wait_recv()
            total = total + part_b[b]
        return total

    def finalize(b, carry):
        total = local_sum(b)
        if me < 2:
            part_push(0, b, part_b, pb_send, pb_sem, me).wait_recv()
            total = total + part_b[b]
        dk_out[b] = (total[0] * scale).astype(BF16)
        dv_out[b] = total[1].astype(BF16)
        return carry

    for t in range(TAIL):
        b = remote_rows + t
        tail_own[t] = local_sum(b)
        if me == 3:
            part_push(1, b, part_a, pa_send, pa_sem, me).wait_recv()
            tail_send[t] = part_a[b]
        else:
            tail_send[t] = jnp.zeros((2, 128, 128), F32) if second_hop is None else ring[b % RING, :, rows(second_hop[0])]
    lax.fori_loop(0, remote_rows, finalize, 0)

    if me > 0:
        for b in range(n_rows - RING, n_rows):
            sent(b)
    if me == 2:
        for e in range(TAIL):
            for move in extra_out(e, 3) + [extra_acc(e, 3)]:
                move.wait_send()
    if me == 3:
        for e in range(TAIL):
            kv_others(remote_rows + e)
            for move in extra_in(e, 2):
                move.wait_send()
            for move in extra_out(e, me):
                move.wait_recv()
    for slot in range(len(direct)):
        for a, src in enumerate((k_hbm, v_hbm)):
            remote(src, kv.at[a, :, own], kv_send.at[2 * slot, a], kv_sem.at[a, 0, 0], me).wait_send()
    if relay is not None:
        for a in range(2):
            remote(kv.at[a, :, rows(relay[0])], kv.at[a, :, own], kv_send.at[1, a], kv_sem.at[a, 0, 0], me).wait_send()


def kernel(n_ctx, n_batch, scale, *refs):
    me = lax.axis_index("ctx")
    barrier = pltpu.get_barrier_semaphore()
    for step in range(1, n_ctx):
        pl.semaphore_signal(barrier, inc=1, device_id={"ctx": lax.rem(me + step, n_ctx)}, device_id_type=MESH)
    pl.semaphore_wait(barrier, n_ctx - 1)
    for i in range(n_ctx):
        pl.when(me == i)(functools.partial(device_program, i, n_batch, scale, refs))


def put(*refs):
    results, outs, sem = refs[:2], refs[2:4], refs[4]
    copies = []
    for i, (result, out) in enumerate(zip(results, outs)):
        n = result.shape[0] // CHUNKS
        for c in range(CHUNKS):
            part = pl.ds(c * n, n)
            copies.append(pltpu.make_async_copy(result.at[part], out.at[part], sem.at[i, c]))
    for copy in copies:
        copy.start()
    for copy in copies:
        copy.wait()


def put_last(scale, dk_main, dv_main, own, received, dk_hbm, dv_hbm, dk_tail, dv_tail, sem):
    n = dk_main.shape[0] - TAIL
    main, tail = pl.ds(0, n), pl.ds(n, TAIL)
    copies = [pltpu.make_async_copy(dk_main.at[main], dk_hbm.at[main], sem.at[0]), pltpu.make_async_copy(dv_main.at[main], dv_hbm.at[main], sem.at[1])]
    for copy in copies:
        copy.start()
    total = own[...] + received[...]
    dk_tail[...] = (total[:, 0] * scale).astype(BF16)
    dv_tail[...] = total[:, 1].astype(BF16)
    last = [pltpu.make_async_copy(dk_tail, dk_hbm.at[tail], sem.at[2]), pltpu.make_async_copy(dv_tail, dv_hbm.at[tail], sem.at[3])]
    for copy in last:
        copy.start()
    for copy in copies + last:
        copy.wait()


def solution(mesh):
    part_spec = P("dp", "ctx")
    n_ctx = mesh.shape["ctx"]

    def local_step(queries, keys, values, grad_out):
        n_batch, c_len, n_q, d_head = queries.shape
        heads = (0, 2, 1, 3)
        q, do = jnp.transpose(queries, heads), jnp.transpose(grad_out, heads)
        k, v = keys.reshape(n_batch, c_len, d_head), values.reshape(n_batch, c_len, d_head)
        width = n_ctx * c_len
        vmem, dma = pltpu.VMEM, pltpu.SemaphoreType.DMA
        scratch = [
            vmem((2, n_batch, width, d_head), BF16),
            vmem((n_batch + 1, 2, c_len, d_head), F32),
            vmem((RING + 1, 2, width - c_len, d_head), F32),
            vmem((n_batch, 2, c_len, d_head), F32),
            vmem((n_batch, 2, c_len, d_head), F32),
        ]
        scratch += [vmem((3, n_q, c_len, d_head), BF16)] * 2
        scratch += [vmem((width, 256), F32)] * 7 + [vmem((width, 256), BF16)] * 5
        scratch += [vmem((2, 8, 256), F32), vmem((3, 8, 256), F32), vmem((2, 8, 256), F32)] + [vmem((3, d_head, width), BF16)] * 2
        scratch += [dma((2,)), dma((2, n_ctx, n_batch)), dma((3, 2)), dma((n_batch,)), dma((n_batch,))] + [dma((RING,))] * 3
        scratch += [dma((3,))] * 2
        scratch += [vmem((TAIL, n_q, c_len, d_head), BF16)] * 2 + [vmem((TAIL + 1, 2, c_len, d_head), F32)]
        scratch += [dma((2, TAIL)), dma((4, TAIL)), dma((2, TAIL)), dma((2, TAIL)), dma((TAIL,))]
        hbm = pl.BlockSpec(memory_space=pl.ANY)
        local = pl.BlockSpec(memory_space=pltpu.VMEM)
        scale = d_head ** -0.5
        tail = (TAIL, 2, c_len, d_head)
        out, grad_q, grad_k, grad_v, tail_send, tail_own = pl.pallas_call(
            functools.partial(kernel, n_ctx, n_batch, scale),
            out_shape=[pltpu.VMEM(x.shape, BF16) for x in (q, q, k, v)] + [pltpu.VMEM(tail, F32), pltpu.VMEM(tail, F32)],
            in_specs=[hbm] * 4,
            out_specs=[local] * 6,
            scratch_shapes=scratch,
            compiler_params=pltpu.CompilerParams(collective_id=0, has_side_effects=True, vmem_limit_bytes=37 * 2 ** 20),
        )(q, do, k, v)
        received = lax.ppermute(tail_send, "ctx", [(2, 0), (3, 1)])
        out, grad_q = pl.pallas_call(
            put,
            out_shape=[jax.ShapeDtypeStruct(q.shape, BF16)] * 2,
            in_specs=[local] * 2,
            out_specs=[hbm] * 2,
            scratch_shapes=[dma((2, CHUNKS))],
            cost_estimate=pl.CostEstimate(flops=10 ** 10, bytes_accessed=2 * q.size * 2, transcendentals=0),
            compiler_params=pltpu.CompilerParams(vmem_limit_bytes=2 ** 20),
        )(out, grad_q)
        grad_k, grad_v = pl.pallas_call(
            functools.partial(put_last, scale),
            out_shape=[jax.ShapeDtypeStruct(k.shape, BF16)] * 2,
            in_specs=[local] * 4,
            out_specs=[hbm] * 2,
            scratch_shapes=[vmem((TAIL, c_len, d_head), BF16)] * 2 + [dma((4,))],
            compiler_params=pltpu.CompilerParams(vmem_limit_bytes=4 * 2 ** 20),
        )(grad_k, grad_v, tail_own, received)
        return jnp.transpose(out, heads), jnp.transpose(grad_q, heads), grad_k.reshape(keys.shape), grad_v.reshape(values.shape)

    return jax.shard_map(local_step, mesh=mesh, in_specs=(part_spec,) * 4, out_specs=(part_spec,) * 4, check_vma=False)
```

```python
import functools

import jax
import jax.numpy as jnp
from jax import lax
from jax.experimental import pallas as pl
from jax.experimental.pallas import tpu as pltpu
from jax.sharding import PartitionSpec as P

F32, BF16 = jnp.float32, jnp.bfloat16
LOG2E = 1.4426950408889634
NEG_BIG = -1e30
MESH = pl.DeviceIdType.MESH
RING = 9
CHUNKS = 4
FLIP_AT = 1
TAIL = 2
PIECE = 32


def dot(a, b):
    return lax.dot_general(a, b, (((1,), (0,)), ((), ())), preferred_element_type=F32)


def remote(src, dst, send_sem, recv_sem, to):
    return pltpu.make_async_remote_copy(src_ref=src, dst_ref=dst, send_sem=send_sem, recv_sem=recv_sem, device_id={"ctx": to}, device_id_type=MESH)


def device_program(me, n_batch, scale, refs):
    (q_hbm, do_hbm, k_hbm, v_hbm, o_out, dq_out, dk_out, dv_out, tail_send, tail_own,
     kv, own_acc, ring, part_a, part_b, q_buf, do_buf,
     s_0, s_1, p_0, p_1, p_2, dp_0, dp_1, ph_0, ph_1, ds_0, ds_1, pb_buf, max_s, inv_s, delta_s, kt, vt,
     own_sem, kv_sem, kv_send, pa_sem, pb_sem, pa_send, pb_send, red_send,
     q_sem, do_sem, x_q, x_do, x_acc, x_sem, x_send, xo_sem, xo_send, xa_send) = refs
    blocks = me + 1
    remote_rows = n_batch - TAIL
    n_rows = remote_rows if me == 3 else n_batch
    s_buf, p_buf, dp_buf, ph_buf, ds_buf = (s_0, s_1), (p_0, p_1, p_2), (dp_0, dp_1), (ph_0, ph_1), (ds_0, ds_1)
    own = pl.ds(me * 128, 128)

    def rows(j):
        return pl.ds(j * 128, 128)

    def own_copy(a, src):
        return pltpu.make_async_copy(src, kv.at[a, :, own], own_sem.at[a])

    def kv_push(a, src, j, b, to, slot):
        return remote(src, kv.at[a, b, rows(j)], kv_send.at[slot, a], kv_sem.at[a, j, b], to)

    def kv_wait(j, b):
        for a in range(2):
            kv_push(a, kv.at[a, b, rows(j)], j, b, me, 0).wait_recv()

    def q_copy(b, slot):
        return pltpu.make_async_copy(q_hbm.at[b], q_buf.at[slot], q_sem.at[slot])

    def do_copy(b, slot):
        return pltpu.make_async_copy(do_hbm.at[b], do_buf.at[slot], do_sem.at[slot])

    def part_push(j, b, dst, send_sem, recv_sem, to):
        slot = lax.rem(b, RING) if not isinstance(b, int) else b % RING
        return remote(ring.at[slot, :, rows(j)], dst.at[b], send_sem.at[slot], recv_sem.at[b], to)

    first_hop = {0: [], 1: [(0, part_a, pa_send, pa_sem, 0)], 2: [(1, part_a, pa_send, pa_sem, 3)], 3: [(0, part_a, pa_send, pa_sem, 2), (2, part_b, pb_send, pb_sem, 2)]}[me]
    second_hop = {0: None, 1: None, 2: (0, 0), 3: (1, 1)}[me]
    relay = {0: None, 1: None, 2: (0, 3), 3: (1, 2)}[me]

    def relay_block(b):
        j, to = relay
        kv_wait(j, b)
        for a in range(2):
            kv_push(a, kv.at[a, b, rows(j)], j, b, to, 1).start()

    def kv_others(b):
        for j in range(me):
            if relay is None or j != relay[0]:
                kv_wait(j, b)

    def extra_in(e, to):
        b = remote_rows + e
        moves = [remote(q_hbm.at[b], x_q.at[e], x_send.at[0, e], x_sem.at[0, e], to), remote(do_hbm.at[b], x_do.at[e], x_send.at[1, e], x_sem.at[1, e], to)]
        for a, src in enumerate((k_hbm, v_hbm)):
            moves.append(remote(src.at[b], kv.at[a, b, rows(3)], x_send.at[2 + a, e], kv_sem.at[a, 3, b], to))
        return moves

    def extra_out(e, to):
        b = remote_rows + e
        return [remote(q_buf.at[e], o_out.at[b], xo_send.at[0, e], xo_sem.at[0, e], to), remote(do_buf.at[e], dq_out.at[b], xo_send.at[1, e], xo_sem.at[1, e], to)]

    def extra_acc(e, to):
        return remote(x_acc.at[e], part_b.at[remote_rows + e], xa_send.at[e], pb_sem.at[remote_rows + e], to)

    direct = {0: (2, 1), 1: (3,), 2: (3,), 3: ()}[me]

    def push_own(b, carry):
        for slot, to in enumerate(direct):
            for a, src in enumerate((k_hbm, v_hbm)):
                kv_push(a, src.at[b], me, b, to, 2 * slot).start()
        return carry

    push_own(0, 0)
    own_copy(0, k_hbm).start()
    own_copy(1, v_hbm).start()
    q_copy(0, 0).start()
    do_copy(0, 0).start()
    if direct:
        lax.fori_loop(1, n_batch, push_own, 0)
    own_copy(0, k_hbm).wait()
    own_copy(1, v_hbm).wait()
    if relay is not None:
        relay_block(0)

    causal_r = lax.broadcasted_iota(jnp.int32, (128, 256), 0)
    causal_c = lax.broadcasted_iota(jnp.int32, (128, 256), 1) & 127

    def pair(ref, slot, x):
        return ref[slot, 2 * x:2 * x + 2].reshape(256, 128)

    def main_acc(j, s3):
        return (own_acc, (s3[1],), True) if j == me else (ring, (s3[2],), True)

    def extra_row_acc(j, s3):
        if j == 3:
            return x_acc, (s3[1] - remote_rows,), True
        return (own_acc, (s3[1],), False) if j == me else (ring, (s3[2],), False)

    main_cfg = (blocks, q_buf, do_buf, o_out, dq_out, 0, main_acc)
    extra_cfg = (blocks + 1, x_q, x_do, q_buf, do_buf, 3, extra_row_acc)

    def sub_step(x, stages, ahead=None, cfg=main_cfg):
        blocks, q_src, do_src, o_dst, dq_dst, at, acc_of = cfg
        width = blocks * 128
        par = [(x - k) % 2 for k in range(5)]
        tri = [(x - k) % 3 for k in range(5)]
        s0, s1, s2, s3, s4 = stages
        if s0 is not None:
            qt0 = pair(q_src, s0[3], s0[5]).T
        if s2 is not None:
            dot2 = pair(do_src, s2[3], s2[5]).T
        if s1 is not None:
            max1 = max_s[par[1], 0:1]
        if s3 is not None:
            q3, do3 = pair(q_src, s3[3], s3[5]), pair(do_src, s3[3], s3[5])
            inv3, delta3 = inv_s[tri[3], 0:1], delta_s[par[3], 0:1]
        max8 = sum8 = None
        for j in range(blocks):
            r = slice(j * 128, j * 128 + 128)
            pieces = [slice(y, y + PIECE) for y in range(j * 128, j * 128 + 128, PIECE)]
            if j == 0 and s2 is not None:
                ot = (dot(vt[s2[4], :, :width], ph_buf[par[2]][:width]) * inv_s[tri[2], 0:1]).astype(BF16)
                o_dst[s2[at], 2 * s2[5]:2 * s2[5] + 2] = ot.T.reshape(2, 128, 128)
                delta_s[par[2], 0:1] = jnp.sum(dot2.astype(F32) * ot.astype(F32), axis=0, keepdims=True)
            if j == min(1, blocks - 1) and s4 is not None:
                dq = (dot(kt[s4[4], :, :width], ds_buf[par[4]][:width]) * scale).astype(BF16)
                dq_dst[s4[at], 2 * s4[5]:2 * s4[5] + 2] = dq.T.reshape(2, 128, 128)
            if s3 is not None:
                for y in pieces:
                    pb = p_buf[tri[3]][y] * inv3
                    ds_buf[par[3]][y] = (pb * (dp_buf[par[3]][y] - delta3)).astype(BF16)
                    pb_buf[y] = pb.astype(BF16)
                dv = dot(pb_buf[r], do3)
                dk = dot(ds_buf[par[3]][r], q3)
                dst, idx, fresh = acc_of(j, s3)
                for w, part in enumerate((dk, dv)):
                    where = idx + ((w,) if dst is not ring else (w, r))
                    dst[where] = part if fresh and s3[5] == 0 else dst[where] + part
            if s0 is not None:
                st = dot(kv[0, s0[0], r], qt0)
                if j == blocks - 1:
                    st = jnp.where(causal_r <= causal_c, st, NEG_BIG)
                s_buf[par[0]][r] = st
                part = jnp.max(st.reshape(16, 8, 256), axis=0)
                max8 = part if max8 is None else jnp.maximum(max8, part)
            if s1 is not None:
                for y in pieces:
                    p = jnp.exp2((s_buf[par[1]][y] - max1) * (scale * LOG2E))
                    p_buf[tri[1]][y] = p
                    ph_buf[par[1]][y] = p.astype(BF16)
                    part = jnp.sum(p.reshape(PIECE // 8, 8, 256), axis=0)
                    sum8 = part if sum8 is None else sum8 + part
            if s2 is not None:
                dp_buf[par[2]][r] = dot(kv[1, s2[0], r], dot2)
            if ahead is not None:
                kt[ahead[1], :, r] = kv[0, ahead[0], r].T
                vt[ahead[1], :, r] = kv[1, ahead[0], r].T
        if s1 is not None:
            inv_s[tri[1], 0:1] = 1.0 / jnp.sum(sum8, axis=0, keepdims=True)
        if s0 is not None:
            max_s[par[0], 0:1] = jnp.max(max8, axis=0, keepdims=True)

    def reduce_part(b):
        j, _ = second_hop
        part_push(j, b, part_a, pa_send, pa_sem, me).wait_recv()
        slot = lax.rem(b, RING) if not isinstance(b, int) else b % RING
        ring[slot, :, rows(j)] += part_a[b]

    def send_reduced(b):
        j, to = second_hop
        part_push(j, b, part_b, red_send, pb_sem, to).start()

    def send_parts(b):
        for j, dst, send_sem, recv_sem, to in first_hop:
            part_push(j, b, dst, send_sem, recv_sem, to).start()

    def sent(b):
        for j, dst, send_sem, recv_sem, to in first_hop:
            part_push(j, b, dst, send_sem, recv_sem, to).wait_send()
        if second_hop is not None and (not isinstance(b, int) or b < remote_rows):
            part_push(second_hop[0], b, part_b, red_send, pb_sem, second_hop[1]).wait_send()

    def paced(b):
        return jnp.maximum(b, 0) if me == 3 else jnp.maximum((82 * (b + 1) - 142) // 100, 0)


    def step(b, carry):
        cur, prev = lax.rem(b, 3), lax.rem(b + 2, 3)
        b_prev = jnp.maximum(b - 1, 0)
        own_prev = jnp.where(b == 0, n_batch, b - 1)
        ring_cur, ring_prev = lax.rem(b, RING), lax.rem(b + RING - 1, RING)

        @pl.when(b + 1 < n_rows)
        def _():
            nxt = lax.rem(b + 1, 3)
            q_copy(b + 1, nxt).start()
            do_copy(b + 1, nxt).start()

        if me > 0:
            pl.when(b >= RING)(lambda: sent(b - RING))

        if relay is not None:

            if me == 2:
                pl.when(b + 1 < n_batch)(lambda: relay_block(b + 1))
            else:
                pl.when((b >= 1) & (2 * b < n_batch))(lambda: relay_block(2 * b))
                pl.when(2 * b + 1 < n_batch)(lambda: relay_block(2 * b + 1))
        kv_others(b)
        q_copy(b, cur).wait()
        do_copy(b, cur).wait()
        for x in range(6):
            here = (b, b, ring_cur, cur, cur)
            before = (b_prev, own_prev, ring_prev, prev, prev)
            sub_step(x, [here + (x - k,) if x >= k else before + (x - k + 6,) for k in range(5)], (b, cur) if x == FLIP_AT else None)
        pl.when((b >= 1) & (b <= remote_rows) if me == 2 else b >= 1)(lambda: send_parts(b - 1))

        if second_hop is not None:

            @pl.when(paced(b) > paced(b - 1))
            def _():
                reduce_part(paced(b) - 1)
                send_reduced(paced(b) - 1)

        if me == 3:

            @pl.when(b < TAIL)
            def _():
                for move in extra_in(b, 2):
                    move.start()

        return carry

    lax.fori_loop(0, n_rows, step, 0)

    last = n_rows - 1
    ls = last % 3
    end = (last, last, last % RING, ls, ls)
    for x in range(3):
        sub_step(x, [end + (x - k + 6,) if k > x else None for k in range(5)])
    if me != 2:
        send_parts(last)
    if me == 3:
        reduce_part(last)
    sub_step(3, [None, None, None, None, end + (5,)])
    if me == 3:
        send_reduced(last)

    def reduce_and_send(b):
        reduce_part(b)
        send_reduced(b)

    if me == 2:
        for b in range((82 * n_batch - 142) // 100, remote_rows - 1 - 2 * TAIL):
            reduce_and_send(b)

        def extra(e, carry):
            b = remote_rows + e
            prev = lax.rem(e + TAIL - 1, TAIL)
            here = (b, b, lax.rem(b, RING), e, e)
            before = (jnp.maximum(b - 1, remote_rows), jnp.where(e == 0, n_batch, b - 1), jnp.where(e == 0, RING, lax.rem(b - 1, RING)), prev, prev)
            for x in range(6):
                sub_step(x, [here + (x - k,) if x >= k else before + (x - k + 6,) for k in range(5)], (b, e) if x == FLIP_AT else None, extra_cfg)

            @pl.when(e >= 1)
            def _():
                for move in extra_out(e - 1, 3):
                    move.start()
                extra_acc(e - 1, 3).start()
                send_parts(b - 1)

            reduce_and_send(remote_rows - 1 - 2 * TAIL + 2 * e)
            reduce_and_send(remote_rows - 2 * TAIL + 2 * e)
            return carry

        for e in range(TAIL):
            for move in extra_in(e, me):
                move.wait_recv()
        lax.fori_loop(0, TAIL, extra, 0)
        end = (n_batch - 1, n_batch - 1, (n_batch - 1) % RING, TAIL - 1, TAIL - 1)
        for x in range(3):
            sub_step(x, [end + (x - k + 6,) if k > x else None for k in range(5)], None, extra_cfg)
        extra_acc(TAIL - 1, 3).start()
        send_parts(n_batch - 1)
        sub_step(3, [None, None, None, None, end + (5,)], None, extra_cfg)
        reduce_and_send(remote_rows - 1)
        for move in extra_out(TAIL - 1, 3):
            move.start()

    def local_sum(b):
        if me == 3 and isinstance(b, int) and b >= remote_rows:
            extra_acc(b - remote_rows, me).wait_recv()
            return part_b[b]
        total = own_acc[b]
        if me == 0:
            part_push(0, b, part_a, pa_send, pa_sem, me).wait_recv()
            total = total + part_a[b]
        if me == 2 and not (isinstance(b, int) and b >= remote_rows):
            part_push(0, b, part_b, pb_send, pb_sem, me).wait_recv()
            total = total + part_b[b]
        return total

    def finalize(b, carry):
        total = local_sum(b)
        if me < 2:
            part_push(0, b, part_b, pb_send, pb_sem, me).wait_recv()
            total = total + part_b[b]
        dk_out[b] = (total[0] * scale).astype(BF16)
        dv_out[b] = total[1].astype(BF16)
        return carry

    for t in range(TAIL):
        b = remote_rows + t
        tail_own[t] = local_sum(b)
        if me == 3:
            part_push(1, b, part_a, pa_send, pa_sem, me).wait_recv()
            tail_send[t] = part_a[b]
        else:
            tail_send[t] = jnp.zeros((2, 128, 128), F32) if second_hop is None else ring[b % RING, :, rows(second_hop[0])]
    lax.fori_loop(0, remote_rows, finalize, 0)

    if me > 0:
        for b in range(n_rows - RING, n_rows):
            sent(b)
    if me == 2:
        for e in range(TAIL):
            for move in extra_out(e, 3) + [extra_acc(e, 3)]:
                move.wait_send()
    if me == 3:
        for e in range(TAIL):
            kv_others(remote_rows + e)
            for move in extra_in(e, 2):
                move.wait_send()
            for move in extra_out(e, me):
                move.wait_recv()
    for slot in range(len(direct)):
        for a, src in enumerate((k_hbm, v_hbm)):
            remote(src, kv.at[a, :, own], kv_send.at[2 * slot, a], kv_sem.at[a, 0, 0], me).wait_send()
    if relay is not None:
        for a in range(2):
            remote(kv.at[a, :, rows(relay[0])], kv.at[a, :, own], kv_send.at[1, a], kv_sem.at[a, 0, 0], me).wait_send()


def kernel(n_ctx, n_batch, scale, *refs):
    me = lax.axis_index("ctx")
    barrier = pltpu.get_barrier_semaphore()
    for step in range(1, n_ctx):
        pl.semaphore_signal(barrier, inc=1, device_id={"ctx": lax.rem(me + step, n_ctx)}, device_id_type=MESH)
    pl.semaphore_wait(barrier, n_ctx - 1)
    for i in range(n_ctx):
        pl.when(me == i)(functools.partial(device_program, i, n_batch, scale, refs))


def put(*refs):
    results, outs, sem = refs[:2], refs[2:4], refs[4]
    copies = []
    for i, (result, out) in enumerate(zip(results, outs)):
        n = result.shape[0] // CHUNKS
        for c in range(CHUNKS):
            part = pl.ds(c * n, n)
            copies.append(pltpu.make_async_copy(result.at[part], out.at[part], sem.at[i, c]))
    for copy in copies:
        copy.start()
    for copy in copies:
        copy.wait()


def put_last(scale, dk_main, dv_main, own, received, dk_hbm, dv_hbm, dk_tail, dv_tail, sem):
    n = dk_main.shape[0] - TAIL
    main, tail = pl.ds(0, n), pl.ds(n, TAIL)
    copies = [pltpu.make_async_copy(dk_main.at[main], dk_hbm.at[main], sem.at[0]), pltpu.make_async_copy(dv_main.at[main], dv_hbm.at[main], sem.at[1])]
    for copy in copies:
        copy.start()
    total = own[...] + received[...]
    dk_tail[...] = (total[:, 0] * scale).astype(BF16)
    dv_tail[...] = total[:, 1].astype(BF16)
    last = [pltpu.make_async_copy(dk_tail, dk_hbm.at[tail], sem.at[2]), pltpu.make_async_copy(dv_tail, dv_hbm.at[tail], sem.at[3])]
    for copy in last:
        copy.start()
    for copy in copies + last:
        copy.wait()


def solution(mesh):
    part_spec = P("dp", "ctx")
    n_ctx = mesh.shape["ctx"]

    def local_step(queries, keys, values, grad_out):
        n_batch, c_len, n_q, d_head = queries.shape
        heads = (0, 2, 1, 3)
        q, do = jnp.transpose(queries, heads), jnp.transpose(grad_out, heads)
        k, v = keys.reshape(n_batch, c_len, d_head), values.reshape(n_batch, c_len, d_head)
        width = n_ctx * c_len
        vmem, dma = pltpu.VMEM, pltpu.SemaphoreType.DMA
        scratch = [
            vmem((2, n_batch, width, d_head), BF16),
            vmem((n_batch + 1, 2, c_len, d_head), F32),
            vmem((RING + 1, 2, width - c_len, d_head), F32),
            vmem((n_batch, 2, c_len, d_head), F32),
            vmem((n_batch, 2, c_len, d_head), F32),
        ]
        scratch += [vmem((3, n_q, c_len, d_head), BF16)] * 2
        scratch += [vmem((width, 256), F32)] * 7 + [vmem((width, 256), BF16)] * 5
        scratch += [vmem((2, 8, 256), F32), vmem((3, 8, 256), F32), vmem((2, 8, 256), F32)] + [vmem((3, d_head, width), BF16)] * 2
        scratch += [dma((2,)), dma((2, n_ctx, n_batch)), dma((3, 2)), dma((n_batch,)), dma((n_batch,))] + [dma((RING,))] * 3
        scratch += [dma((3,))] * 2
        scratch += [vmem((TAIL, n_q, c_len, d_head), BF16)] * 2 + [vmem((TAIL + 1, 2, c_len, d_head), F32)]
        scratch += [dma((2, TAIL)), dma((4, TAIL)), dma((2, TAIL)), dma((2, TAIL)), dma((TAIL,))]
        hbm = pl.BlockSpec(memory_space=pl.ANY)
        local = pl.BlockSpec(memory_space=pltpu.VMEM)
        scale = d_head ** -0.5
        tail = (TAIL, 2, c_len, d_head)
        out, grad_q, grad_k, grad_v, tail_send, tail_own = pl.pallas_call(
            functools.partial(kernel, n_ctx, n_batch, scale),
            out_shape=[pltpu.VMEM(x.shape, BF16) for x in (q, q, k, v)] + [pltpu.VMEM(tail, F32), pltpu.VMEM(tail, F32)],
            in_specs=[hbm] * 4,
            out_specs=[local] * 6,
            scratch_shapes=scratch,
            compiler_params=pltpu.CompilerParams(collective_id=0, has_side_effects=True, vmem_limit_bytes=37 * 2 ** 20),
        )(q, do, k, v)
        received = lax.ppermute(tail_send, "ctx", [(2, 0), (3, 1)])
        out, grad_q = pl.pallas_call(
            put,
            out_shape=[jax.ShapeDtypeStruct(q.shape, BF16)] * 2,
            in_specs=[local] * 2,
            out_specs=[hbm] * 2,
            scratch_shapes=[dma((2, CHUNKS))],
            cost_estimate=pl.CostEstimate(flops=10 ** 10, bytes_accessed=2 * q.size * 2, transcendentals=0),
            compiler_params=pltpu.CompilerParams(vmem_limit_bytes=2 ** 20),
        )(out, grad_q)
        grad_k, grad_v = pl.pallas_call(
            functools.partial(put_last, scale),
            out_shape=[jax.ShapeDtypeStruct(k.shape, BF16)] * 2,
            in_specs=[local] * 4,
            out_specs=[hbm] * 2,
            scratch_shapes=[vmem((TAIL, c_len, d_head), BF16)] * 2 + [dma((4,))],
            compiler_params=pltpu.CompilerParams(vmem_limit_bytes=4 * 2 ** 20),
        )(grad_k, grad_v, tail_own, received)
        return jnp.transpose(out, heads), jnp.transpose(grad_q, heads), grad_k.reshape(keys.shape), grad_v.reshape(values.shape)

    return jax.shard_map(local_step, mesh=mesh, in_specs=(part_spec,) * 4, out_specs=(part_spec,) * 4, check_vma=False)
```
